32 devices in a mesh: level: 2 (over x), subj: 4 (over y, core), gz: 4 (over z).
Axes of the slice: x: 2, y: 2, z: 4, core: 2. Of those that a mesh axis runs over, the one named last changes fastest.
Arguments:
- images: bfloat16 [8, 192, 192, 192], P('subj', 'gz'), may hold values from -6 to 6
- momenta: float32 [8, 96, 3, 96, 96], P('subj', 'gz'), may hold values from -18 to 18
- assign: int32 [8], replicated, may hold values from 0 to 7, as said below
Outputs:
- template: float32 [192, 192, 192], P('gz')
The draws below stay inside these ranges and needn't reach their ends.
Inputs may be any that keep to these rules, and one draw needn't show every extreme that they name: assign is a permutation of 0 to 7 with assign[i] % 2 == i % 2 for every i.
All inputs are finite; a program needn't handle non-finite values.
Results may differ from the reference program's by a relative error of at most 0.00069.
Values may be sent and summed in bfloat16 or wider, within the bound.
A program may use at most 128 MiB of HBM per device.

```python
import jax
import jax.numpy as jnp
from jax import lax

NF = 192
NC = 96
SUBJ_DEV = 2
SWEEPS = 2
SUBJECTS = 8


def draw_assign(key, part):
    groups = SUBJECTS // SUBJ_DEV
    keys = jax.random.split(jax.random.fold_in(key, 7), SUBJ_DEV)
    orders = jax.vmap(lambda single: jax.random.permutation(single, groups))(keys)
    slots = jnp.arange(SUBJ_DEV, dtype=jnp.int32)
    table = orders.T.astype(jnp.int32) * SUBJ_DEV + slots[None, :]
    return table.reshape(SUBJECTS)


def block_levels(stream_key, dims, cuts, smallest, largest):
    level, own = 1.0, jax.random.fold_in(stream_key, 6)
    for position, parts in cuts:
        draws = jnp.exp(jax.random.uniform(jax.random.fold_in(own, position), (parts,), jnp.float32, smallest / len(cuts), largest / len(cuts)))
        level = level * jnp.repeat(draws, dims[position] // parts).reshape([-1 if axis == position else 1 for axis in range(len(dims))])
    return level


def bell_draw(stream_key, extent, deviation, limit, cuts=(), kind=jnp.bfloat16):
    entries = jax.random.normal(stream_key, extent, jnp.float32) * deviation
    if len(cuts) > 0:
        entries = block_levels(stream_key, extent, cuts, -0.22, 0.18) * entries
    return jnp.clip(entries, min=-limit, max=limit).astype(kind)


def setup_inputs(seed: int = 0) -> dict:
    key_of = jax.random.split(jax.random.key(seed), 4)
    return {
        "images": bell_draw(key_of[0], (SUBJECTS, NF, NF, NF), 1.0, 6.0, ((0, 4), (1, 4))),
        "momenta": bell_draw(key_of[1], (SUBJECTS, NC, 3, NC, NC), 3.0, 18.0, ((0, 4), (1, 4)), jnp.float32),
        "assign": draw_assign(jax.random.fold_in(key_of[3], 71), 0),
    }


def band(padded, count, axis):
    def take(offset):
        return lax.slice_in_dim(padded, offset, offset + count, axis=axis)
    return (take(0) + take(4)) * 0.0625 + (take(1) + take(3)) * 0.25 + take(2) * 0.375


def blur_plane(field, axis):
    widths = [(2, 2) if dimension == axis else (0, 0) for dimension in range(field.ndim)]
    return band(jnp.pad(field, widths), field.shape[axis], axis)


def upsample_table(finest, coarse, offset):
    rows_fine = jnp.arange(finest, dtype=jnp.int32)[:, None]
    columns = jnp.arange(coarse, dtype=jnp.int32)[None, :]
    nearest = rows_fine // 2 + offset
    farther = nearest + 2 * (rows_fine % 2) - 1
    return 0.75 * (columns == nearest).astype(jnp.float32) + 0.25 * (columns == farther).astype(jnp.float32)


def warp_slab(extended, upsampled):
    center = extended[1:-1]
    grad_z = (extended[2:] - extended[:-2]) * 0.5
    padded_y = jnp.pad(center, ((0, 0), (1, 1), (0, 0)))
    grad_y = (padded_y[:, 2:] - padded_y[:, :-2]) * 0.5
    padded_x = jnp.pad(center, ((0, 0), (0, 0), (1, 1)))
    grad_x = (padded_x[:, :, 2:] - padded_x[:, :, :-2]) * 0.5
    return center - (upsampled[:, 0] * grad_x + upsampled[:, 1] * grad_y + upsampled[:, 2] * grad_z)


def relax(extended):
    center = extended[1:-1]
    padded_y = jnp.pad(center, ((0, 0), (1, 1), (0, 0)))
    padded_x = jnp.pad(center, ((0, 0), (0, 0), (1, 1)))
    neighbours = extended[2:] + extended[:-2] + padded_y[:, 2:] + padded_y[:, :-2] + padded_x[:, :, 2:] + padded_x[:, :, :-2]
    return center + 0.15 * (neighbours - 6.0 * center)


def reference(images, momenta, assign):
    table = upsample_table(NF, NC, 0)
    highest = lax.Precision.HIGHEST

    def per_subject(total, element):
        image, source = element
        moment = lax.dynamic_index_in_dim(momenta, source, 0, keepdims=False)
        smooth = blur_plane(blur_plane(blur_plane(moment, 3), 2), 0)
        coarse_field = smooth.astype(jnp.bfloat16).astype(jnp.float32)
        section_x = jnp.einsum('zcyx,Xx->zcyX', coarse_field, table, precision=highest)
        section_y = jnp.einsum('zcyX,Yy->zcYX', section_x, table, precision=highest)
        upsampled = jnp.einsum('zcYX,Zz->ZcYX', section_y, table, precision=highest)
        extended = jnp.pad(image.astype(jnp.float32), ((1, 1), (0, 0), (0, 0)))
        return total + warp_slab(extended, upsampled), None

    start_total = jnp.zeros((NF, NF, NF), jnp.float32)
    total, _ = lax.scan(per_subject, start_total, (images, assign))
    mean = total / SUBJECTS
    for repeat in range(SWEEPS):
        mean = relax(jnp.pad(mean, ((1, 1), (0, 0), (0, 0))))
    return mean
```

```python
import functools

import jax
import jax.numpy as jnp
from jax import lax
from jax.experimental import pallas as pl
from jax.experimental.pallas import tpu as pltpu
from jax.sharding import PartitionSpec as P

LANES = 128
MARGIN = 8
TOP = 32767.0
F32 = jnp.float32
BF16 = jnp.bfloat16


def upsample_table(finest, coarse):
    rows_fine = jnp.arange(finest, dtype=jnp.int32)[:, None]
    columns = jnp.arange(coarse, dtype=jnp.int32)[None, :]
    nearest = rows_fine // 2
    farther = nearest + 2 * (rows_fine % 2) - 1
    return 0.75 * (columns == nearest).astype(F32) + 0.25 * (columns == farther).astype(F32)


def slope_table(finest):
    rows = jnp.arange(finest, dtype=jnp.int32)[:, None]
    columns = jnp.arange(finest, dtype=jnp.int32)[None, :]
    ahead = (columns == rows + 1).astype(F32)
    behind = (columns == rows - 1).astype(F32)
    return ((ahead - behind) * 0.5).astype(BF16)


def blur_table(coarse):
    rows = jnp.arange(coarse, dtype=jnp.int32)[:, None]
    columns = jnp.arange(coarse, dtype=jnp.int32)[None, :]
    gap = jnp.abs(rows - columns)
    return (
        0.375 * (gap == 0).astype(F32)
        + 0.25 * (gap == 1).astype(F32)
        + 0.0625 * (gap == 2).astype(F32)
    ).astype(BF16)


def split(value):
    high = value.astype(BF16)
    low = (value - high.astype(F32)).astype(BF16)
    return jnp.concatenate([high, low], axis=0)


def dot(a, b):
    return jnp.dot(a, b, preferred_element_type=F32)


def encode(packed):
    peak = jnp.max(jnp.abs(packed), axis=0, keepdims=True)
    peak = jnp.maximum(peak, 1e-30)
    code = jnp.floor(packed * (TOP / peak) + 0.5).astype(jnp.int16)
    return code, jnp.broadcast_to(peak * (1.0 / TOP), (8, LANES))


def fused_kernel(
    sel, images, momenta, up_x, up_y, slope_x, slope_y, blur_x, blur_y,
    codes, scales,
    ext, img, vel, fine, part, peer, ycode, yscale, mean, second, packed,
    rescode, resscale, xcode, xscale,
    lsem, hsend, hrecv, vsend, vrecv, psend, precv, ysend, yrecv, msend, mrecv,
    gsend, grecv, xsend, xrecv, osem,
):
    level = lax.axis_index("level")
    group = lax.axis_index("subj")
    zone = lax.axis_index("gz")
    groups = lax.axis_size("subj")
    zones = lax.axis_size("gz")
    chips = groups // 2
    chip = group // 2
    core = group % 2
    partner = 2 * chip + 1 - core
    up = level
    fine_slab, finest = images.shape[1], images.shape[2]
    slab, coarse = momenta.shape[1], momenta.shape[3]
    rows_half, planes_half = slab // 2, fine_slab // 2
    pairs = (rows_half + 2) // 2
    rows_block, planes_block = rows_half // 2, planes_half // 2
    half = finest // 2
    rest = finest - LANES
    piece = LANES - coarse

    to_zone = zone + 1 - 2 * level
    has_to = (to_zone >= 0) & (to_zone < zones)
    from_zone = zone - 1 + 2 * level
    has_from = (from_zone >= 0) & (from_zone < zones)
    far_step = 2 * core - 1
    crosses = level == core
    far_zone = jnp.where(crosses, zone + far_step, zone)
    has_far = (far_zone >= 0) & (far_zone < zones)
    me = (level, group, zone)
    mate = (level, partner, zone)
    across = (1 - level, group, zone)
    far = (1 - level, partner, far_zone)
    upper = (level, group, to_zone)
    lower = (level, group, from_zone)
    peers = [(chip + d) % chips for d in range(1, chips)]

    def remote(src, dst, send, recv, device):
        return pltpu.make_async_remote_copy(
            src_ref=src, dst_ref=dst, send_sem=send, recv_sem=recv,
            device_id=device, device_id_type=pl.DeviceIdType.MESH,
        )

    load_mom = pltpu.make_async_copy(
        momenta.at[:, pl.ds(level * (rows_half - 3), rows_half + 3)],
        ext.at[:, pl.ds(3 - 3 * level, rows_half + 3)],
        lsem.at[0],
    )
    load_img = pltpu.make_async_copy(
        images.at[:, pl.ds(level * (planes_half - 1), planes_half + 1)],
        img.at[:, pl.ds(1 - level, planes_half + 1)],
        lsem.at[1],
    )
    load_mom.start()
    load_img.start()
    zero_plane = jnp.zeros(mean.shape[1:], F32)

    def clear(j, _):
        mean[j] = zero_plane
        second[j] = zero_plane
        return 0

    lax.fori_loop(0, planes_block + 4, clear, 0)

    barrier = pltpu.get_barrier_semaphore()

    def greet(device):
        pl.semaphore_signal(
            barrier, inc=1, device_id=device, device_id_type=pl.DeviceIdType.MESH
        )

    greet(mate)
    greet(across)
    for other in peers:
        greet((level, 2 * other + core, zone))

    @pl.when(has_to)
    def _():
        greet(upper)

    @pl.when(has_from)
    def _():
        greet(lower)

    @pl.when(has_far)
    def _():
        greet(far)

    pl.semaphore_wait(
        barrier,
        2 + len(peers)
        + has_to.astype(jnp.int32) + has_from.astype(jnp.int32) + has_far.astype(jnp.int32),
    )

    halo_mom = remote(
        momenta.at[:, pl.ds((1 - level) * (slab - 3), 3)],
        ext.at[:, pl.ds(level * (rows_half + 3), 3)],
        hsend.at[0], hrecv.at[0], upper,
    )
    halo_img = remote(
        images.at[:, pl.ds((1 - level) * (fine_slab - 1), 1)],
        img.at[:, pl.ds(level * (planes_half + 1), 1)],
        hsend.at[1], hrecv.at[1], upper,
    )

    @pl.when(has_to)
    def _():
        halo_mom.start()
        halo_img.start()

    @pl.when(jnp.logical_not(has_from))
    def _():
        for s in range(2):
            for e in range(3):
                for k in range(3):
                    ext[s, level * (rows_half + 3) + e, k] = jnp.zeros((coarse, coarse), F32)
            img[s, level * (planes_half + 1)] = jnp.zeros((finest, finest), BF16)

    load_mom.wait()

    def pair_of(i):
        return i + (1 - up) * (pairs - 1 - 2 * i)

    lane = lax.broadcasted_iota(jnp.int32, (coarse, LANES), 1)

    def velocity_sends(t):
        sends = [
            remote(
                vel.at[t, group], vel.at[t, group], vsend.at[t, 0], vrecv.at[t, group], mate
            )
        ]
        for n, other in enumerate(peers):
            sends.append(
                remote(
                    vel.at[t, group], vel.at[t, group], vsend.at[t, 1 + n],
                    vrecv.at[t, group], (level, 2 * other + core, zone),
                )
            )
        return sends

    def relay_sends(t):
        sends = []
        for n, other in enumerate(peers):
            there = 2 * other + core
            sends.append(
                remote(
                    vel.at[t, there], vel.at[t, there], vsend.at[t, chips + n],
                    vrecv.at[t, there], mate,
                )
            )
        return sends

    def smooth(i, _):
        t = pair_of(i)

        @pl.when((i == pairs - 2) & has_from)
        def _():
            halo_mom.wait_recv()

        planes = {}
        for r in range(2):
            row = zone * slab + level * rows_half - 1 + 2 * t + r
            keep = ((row >= 0) & (row < slab * zones)).astype(F32)
            for s in range(2):
                for k in range(3):
                    f = [ext[s, 2 * t + r + o, k] for o in range(5)]
                    value = (f[0] + f[4]) * 0.0625 + (f[1] + f[3]) * 0.25 + f[2] * 0.375
                    wide = dot(split(value), blur_x[...])
                    wide = (wide[:coarse] + wide[coarse:]) * keep
                    planes[6 * r + 3 * s + k] = dot(blur_y[...], split(wide))
        for m in range(3):
            for j in range(3):
                turned = pltpu.roll(planes[9 + m], coarse - piece * j, 1)
                joined = jnp.where(lane < coarse, planes[3 * m + j], turned)
                vel[t, group, 3 * m + j] = joined.astype(BF16)

        @pl.when(i > 0)
        def _():
            for send in velocity_sends(pair_of(i - 1)):
                send.start()

        return 0

    lax.fori_loop(0, pairs, smooth, 0)
    for send in velocity_sends(pair_of(pairs - 1)):
        send.start()

    load_img.wait()

    @pl.when(has_from)
    def _():
        halo_img.wait_recv()

    def relay(t):
        for send in relay_sends(t):
            send.wait_recv()
            send.start()

    def pick(t, source, first, count):
        value = vel[t, 0, first : first + count]
        for other in range(1, groups):
            value = jnp.where(source == other, vel[t, other, first : first + count], value)
        return value

    def raise_row(t, r, s, source):
        slot = lax.rem(2 * t + r, 4)
        if 6 * r + 3 * s < 9:
            chosen = pick(t, source, 6 * r + 3 * s, 3).reshape(3 * coarse, LANES)
            wide = dot(chosen, up_x[0])
            parts = [wide[coarse * k : coarse * (k + 1)] for k in range(3)]
        else:
            chosen = pick(t, source, 0, 9)
            parts = []
            for k in range(3):
                total = dot(chosen[3 * k], up_x[1])
                for j in range(1, 3):
                    total = total + dot(chosen[3 * k + j], up_x[1 + j])
                parts.append(total)
        for k in range(3):
            fine[s, slot, k] = dot(up_y[...], split(parts[k]))

    chunk = finest // 4

    def warp_plane(row, z):
        middle = lax.rem(row, 4)
        outer = lax.rem(row + 3 + 2 * z, 4)
        plane = 2 * (row - 1) + z
        for r in range(0, finest, chunk):
            rows = pl.ds(r, chunk)
            total = None
            for s in range(2):
                image = img[s, plane + 1, rows, :]
                dx = dot(image, slope_x[...])
                dy = dot(slope_y[rows, :], img[s, plane + 1])
                back = img[s, plane, rows, :].astype(F32)
                ahead = img[s, plane + 2, rows, :].astype(F32)
                dz = (ahead - back) * 0.5
                near = (
                    fine[s, middle, 0, rows, :] * dx
                    + fine[s, middle, 1, rows, :] * dy
                    + fine[s, middle, 2, rows, :] * dz
                )
                side = (
                    fine[s, outer, 0, rows, :] * dx
                    + fine[s, outer, 1, rows, :] * dy
                    + fine[s, outer, 2, rows, :] * dz
                )
                value = image.astype(F32) - (0.75 * near + 0.25 * side)
                total = value if total is None else total + value
            part[plane, rows, :] = total[:, :LANES]
            place = rest * (r // half)
            part[plane, pl.ds(finest + r % half, chunk), place : place + rest] = total[:, LANES:]

    def chip_send(row):
        here = lax.rem(row, rows_block)
        return remote(
            part.at[pl.ds(2 * row, 2)], peer.at[pl.ds(2 * here, 2)],
            psend.at[here], precv.at[here], mate,
        )

    def sum_sends(here):
        sends = []
        for n, other in enumerate(peers):
            there = (level, 2 * other + core, zone)
            at = pl.ds(2 * here, 2)
            sends.append(
                remote(
                    ycode.at[chip, at], ycode.at[chip, at], ysend.at[0, here, n],
                    yrecv.at[0, here, chip], there,
                )
            )
            sends.append(
                remote(
                    yscale.at[chip, at], yscale.at[chip, at], ysend.at[1, here, n],
                    yrecv.at[1, here, chip], there,
                )
            )
        return sends

    def settle(row):
        here = lax.rem(row, rows_block)
        chip_send(row).wait_recv()
        for z in range(2):
            code, scale = encode(part[2 * row + z] + peer[2 * here + z])
            ycode[chip, 2 * here + z] = code
            yscale[chip, 2 * here + z] = scale
        for send in sum_sends(here):
            send.start()

    def row_at(n):
        return n + (1 - up) * (rows_half - 1 - 2 * n)

    def owned(row):
        return (row // rows_block) == core

    relay(pair_of(0))

    def main(i, _):
        t = pair_of(i)
        for other in range(chips):
            theirs = 2 * other + 1 - core
            remote(
                vel.at[t, theirs], vel.at[t, theirs], vsend.at[t, 0], vrecv.at[t, theirs], mate
            ).wait_recv()
        for r in range(2):
            for s in range(2):
                raise_row(t, r, s, sel[s])

        @pl.when(i < pairs - 1)
        def _():
            relay(pair_of(i + 1))

        @pl.when(i >= 1)
        def _():
            def step(w, _):
                n = 2 * (i - 1) + w // 2
                row = row_at(n)
                warp_plane(row + 1, lax.rem(w, 2))

                @pl.when(lax.rem(w, 2) == 1)
                def _():
                    @pl.when(jnp.logical_not(owned(row)))
                    def _():
                        chip_send(row).start()

                    prior = row_at(jnp.maximum(n - 1, 0))

                    @pl.when((n > 0) & owned(prior))
                    def _():
                        settle(prior)

                return 0

            lax.fori_loop(0, 4, step, 0)

        return 0

    lax.fori_loop(0, pairs, main, 0)
    final_row = row_at(rows_half - 1)

    @pl.when(owned(final_row))
    def _():
        settle(final_row)

    subjects = 2 * groups

    def enter(n, _):
        here = n + (1 - up) * (rows_block - 1 - 2 * n)
        at = pl.ds(2 * here, 2)
        for other in peers:
            remote(
                ycode.at[other, at], ycode.at[other, at], ysend.at[0, here, 0],
                yrecv.at[0, here, other], me,
            ).wait_recv()
            remote(
                yscale.at[other, at], yscale.at[other, at], ysend.at[1, here, 0],
                yrecv.at[1, here, other], me,
            ).wait_recv()
        for z in range(2):
            plane = 2 * here + z
            value = ycode[0, plane].astype(F32) * yscale[0, plane][:1]
            for other in range(1, chips):
                value = value + ycode[other, plane].astype(F32) * yscale[other, plane][:1]
            value = value * (1.0 / subjects)
            mean[2 + plane, pl.ds(MARGIN, finest), 0:LANES] = value[:finest]
            side = value[finest:]
            mean[2 + plane, pl.ds(MARGIN, half), LANES:finest] = side[:, :rest]
            turned = pltpu.roll(side, LANES - rest, 1)
            mean[2 + plane, pl.ds(MARGIN + half, half), LANES:finest] = turned[:, :rest]
        return 0

    lax.fori_loop(0, rows_block, enter, 0)

    inner_from = 2 + core * 0 + (1 - core) * (planes_block - 2)
    inner_to = core * 0 + (1 - core) * 0 + core * (planes_block + 2)
    outer_from = 2 + core * (planes_block - 2)
    outer_to = (1 - core) * (planes_block + 2)
    edge_mate = remote(
        mean.at[pl.ds(inner_from, 2)], mean.at[pl.ds(inner_to, 2)],
        msend.at[0], mrecv.at[0], mate,
    )
    edge_far = remote(
        mean.at[pl.ds(outer_from, 2)], mean.at[pl.ds(outer_to, 2)],
        msend.at[1], mrecv.at[1], far,
    )

    @pl.when(has_far)
    def _():
        edge_far.start()

    edge_mate.start()
    edge_mate.wait_recv()

    @pl.when(has_far)
    def _():
        edge_far.wait_recv()

    step_rows = finest // 3

    def relax(ref, slot, r):
        rows = pl.ds(MARGIN + r, step_rows)
        center = ref[slot, rows, :]
        width = center.shape[1]
        neighbours = (
            ref[slot - 1, rows, :]
            + ref[slot + 1, rows, :]
            + ref[slot, pl.ds(MARGIN + r - 1, step_rows), :]
            + ref[slot, pl.ds(MARGIN + r + 1, step_rows), :]
            + pltpu.roll(center, 1, 1)
            + pltpu.roll(center, width - 1, 1)
        )
        return center + 0.15 * (neighbours - 6.0 * center)

    low_edge = (core == 0) & jnp.logical_not(has_far)
    high_edge = (core == 1) & jnp.logical_not(has_far)

    def first_sweep(j, _):
        drop = ((j == 1) & low_edge) | ((j == planes_block + 2) & high_edge)
        keep = jnp.where(drop, 0.0, 1.0)
        for r in range(0, finest, step_rows):
            value = relax(mean, j, r) * keep
            second[j, pl.ds(MARGIN + r, step_rows), 0:finest] = value[:, :finest]
        return 0

    lax.fori_loop(1, planes_block + 3, first_sweep, 0)

    base = (2 * level + core) * planes_block
    away = (2 * (1 - level) + core) * planes_block

    def result_sends(j):
        at = pl.ds(j, 1)
        out = codes.at[pl.ds(base + j, 1)]
        return [
            remote(rescode.at[at], xcode.at[at], xsend.at[j], xrecv.at[j], across),
            remote(rescode.at[at], out, gsend.at[0, j], grecv.at[0, j], mate),
            pltpu.make_async_copy(rescode.at[at], out, osem.at[0, j]),
        ]

    def second_sweep(j, _):
        parts = []
        for r in range(0, finest, step_rows):
            value = relax(second, j + 2, r)
            packed[pl.ds(r, step_rows), :] = value[:, :LANES]
            parts.append(value[:, LANES:finest])
        side = jnp.concatenate(parts, axis=0)
        packed[pl.ds(finest, half), 0:rest] = side[:half]
        packed[pl.ds(finest, half), rest:LANES] = side[half:]
        code, scale = encode(packed[...])
        rescode[j] = code
        resscale[j] = scale

        @pl.when(j > 0)
        def _():
            for send in result_sends(j - 1):
                send.start()

        return 0

    lax.fori_loop(0, planes_block, second_sweep, 0)
    for send in result_sends(planes_block - 1):
        send.start()
    scale_out = scales.at[pl.ds(base, planes_block)]
    scale_sends = [
        remote(resscale, xscale, xsend.at[planes_block], xrecv.at[planes_block], across),
        remote(resscale, scale_out, gsend.at[0, planes_block], grecv.at[0, planes_block], mate),
        pltpu.make_async_copy(resscale, scale_out, osem.at[0, planes_block]),
    ]
    for send in scale_sends:
        send.start()

    def hand_sends(j):
        at = pl.ds(j, 1)
        out = codes.at[pl.ds(away + j, 1)]
        return [
            remote(xcode.at[at], out, gsend.at[1, j], grecv.at[1, j], mate),
            pltpu.make_async_copy(xcode.at[at], out, osem.at[1, j]),
        ]

    def hand(j, _):
        result_sends(j)[0].wait_recv()
        for send in hand_sends(j):
            send.start()
        return 0

    lax.fori_loop(0, planes_block, hand, 0)
    scale_away = scales.at[pl.ds(away, planes_block)]
    scale_hands = [
        remote(xscale, scale_away, gsend.at[1, planes_block], grecv.at[1, planes_block], mate),
        pltpu.make_async_copy(xscale, scale_away, osem.at[1, planes_block]),
    ]
    scale_sends[0].wait_recv()
    for send in scale_hands:
        send.start()

    @pl.when(has_to)
    def _():
        halo_mom.wait_send()
        halo_img.wait_send()

    def drain_velocity(t, _):
        for send in velocity_sends(t) + relay_sends(t):
            send.wait_send()
        return 0

    lax.fori_loop(0, pairs, drain_velocity, 0)

    def drain_rows(here, _):
        chip_send((1 - core) * rows_block + here).wait_send()
        for send in sum_sends(here):
            send.wait_send()
        return 0

    lax.fori_loop(0, rows_block, drain_rows, 0)
    edge_mate.wait_send()

    @pl.when(has_far)
    def _():
        edge_far.wait_send()

    def drain_results(j, _):
        cross, over, local = result_sends(j)
        cross.wait_send()
        over.wait()
        local.wait()
        over, local = hand_sends(j)
        over.wait()
        local.wait()
        return 0

    lax.fori_loop(0, planes_block, drain_results, 0)
    scale_sends[0].wait_send()
    scale_sends[1].wait()
    scale_sends[2].wait()
    scale_hands[0].wait()
    scale_hands[1].wait()


def fused(sel, images, momenta):
    groups = lax.axis_size("subj")
    chips = groups // 2
    fine_slab, finest = images.shape[1], images.shape[2]
    slab, coarse = momenta.shape[1], momenta.shape[3]
    rows_half, planes_half = slab // 2, fine_slab // 2
    pairs = (rows_half + 2) // 2
    rows_block, planes_block = rows_half // 2, planes_half // 2
    tall = finest + finest // 2
    piece = LANES - coarse
    table = upsample_table(finest, coarse).astype(BF16)
    columns = table.T
    up_x = [jnp.pad(columns, ((0, piece), (0, 0)))]
    for i in range(0, coarse, piece):
        up_x.append(jnp.pad(columns[i : i + piece], ((coarse, 0), (0, 0))))
    up_x = jnp.stack(up_x)
    up_y = jnp.concatenate([table, table], axis=1)
    slope = slope_table(finest)
    blur = blur_table(coarse)
    blur_x = jnp.pad(blur, ((0, 0), (0, piece)))
    blur_y = jnp.concatenate([blur, blur], axis=1)
    width = -(-(finest + 1) // LANES) * LANES
    dma = pltpu.SemaphoreType.DMA
    vmem = pl.BlockSpec(memory_space=pltpu.VMEM)
    hbm = pl.BlockSpec(memory_space=pl.ANY)
    volume = (planes_block + 4, finest + 2 * MARGIN, width)
    scratch = [
        pltpu.VMEM((2, rows_half + 6, 3, coarse, coarse), F32),
        pltpu.VMEM((2, planes_half + 2, finest, finest), BF16),
        pltpu.VMEM((pairs, groups, 9, coarse, LANES), BF16),
        pltpu.VMEM((2, 4, 3, finest, finest), F32),
        pltpu.VMEM((planes_half, tall, LANES), F32),
        pltpu.VMEM((planes_block, tall, LANES), F32),
        pltpu.VMEM((chips, planes_block, tall, LANES), jnp.int16),
        pltpu.VMEM((chips, planes_block, 8, LANES), F32),
        pltpu.VMEM(volume, F32),
        pltpu.VMEM(volume, F32),
        pltpu.VMEM((tall, LANES), F32),
        pltpu.VMEM((planes_block, tall, LANES), jnp.int16),
        pltpu.VMEM((planes_block, 8, LANES), F32),
        pltpu.VMEM((planes_block, tall, LANES), jnp.int16),
        pltpu.VMEM((planes_block, 8, LANES), F32),
        dma((2,)),
        dma((2,)),
        dma((2,)),
        dma((pairs, 2 * chips)),
        dma((pairs, groups)),
        dma((rows_block,)),
        dma((rows_block,)),
        dma((2, rows_block, max(chips - 1, 1))),
        dma((2, rows_block, chips)),
        dma((2,)),
        dma((2,)),
        dma((2, planes_block + 1)),
        dma((2, planes_block + 1)),
        dma((planes_block + 1,)),
        dma((planes_block + 1,)),
        dma((2, planes_block + 1)),
    ]
    return pl.pallas_call(
        fused_kernel,
        out_shape=(
            jax.ShapeDtypeStruct((fine_slab, tall, LANES), jnp.int16),
            jax.ShapeDtypeStruct((fine_slab, 8, LANES), F32),
        ),
        in_specs=[pl.BlockSpec(memory_space=pltpu.SMEM), hbm, hbm] + [vmem] * 6,
        out_specs=(hbm, hbm),
        scratch_shapes=scratch,
        compiler_params=pltpu.CompilerParams(
            collective_id=0, has_side_effects=True, vmem_limit_bytes=60 * 1024 * 1024
        ),
    )(sel, images, momenta, up_x, up_y, slope.T, slope, blur_x, blur_y)


def decode_kernel(codes, scales, out):
    finest = out.shape[1]
    half = finest // 2
    rest = finest - LANES
    for z in range(out.shape[0]):
        value = codes[z].astype(F32) * scales[z][:1]
        out[z, :, 0:LANES] = value[:finest]
        side = value[finest:]
        out[z, 0:half, LANES:finest] = side[:, :rest]
        turned = pltpu.roll(side, LANES - rest, 1)
        out[z, half:finest, LANES:finest] = turned[:, :rest]


def decode(codes, scales, finest):
    planes, tall = codes.shape[0], codes.shape[1]
    block = 4
    return pl.pallas_call(
        decode_kernel,
        grid=(planes // block,),
        in_specs=[
            pl.BlockSpec((block, tall, LANES), lambda j: (j, 0, 0)),
            pl.BlockSpec((block, 8, LANES), lambda j: (j, 0, 0)),
        ],
        out_specs=pl.BlockSpec((block, finest, finest), lambda j: (j, 0, 0)),
        out_shape=jax.ShapeDtypeStruct((planes, finest, finest), F32),
        compiler_params=pltpu.CompilerParams(dimension_semantics=("arbitrary",)),
    )(codes, scales)


def shards(images, momenta, assign):
    count = momenta.shape[0]
    group = lax.axis_index("subj")
    sel = lax.dynamic_slice_in_dim(assign, group * count, count, 0) // count
    codes, scales = fused(sel.astype(jnp.int32), images, momenta)
    return decode(codes, scales, images.shape[2])


def solution(mesh):
    return jax.shard_map(
        shards,
        mesh=mesh,
        in_specs=(P("subj", "gz", None, None), P("subj", "gz", None, None, None), P()),
        out_specs=P("gz", None, None),
        check_vma=False,
    )
```

```python
import functools

import jax
import jax.numpy as jnp
from jax import lax
from jax.experimental import pallas as pl
from jax.experimental.pallas import tpu as pltpu
from jax.sharding import PartitionSpec as P

LANES = 128
MARGIN = 8
TOP = 32767.0
F32 = jnp.float32
BF16 = jnp.bfloat16


def split(value):
    high = value.astype(BF16)
    low = (value - high.astype(F32)).astype(BF16)
    return jnp.concatenate([high, low], axis=0)


def dot(a, b):
    return jnp.dot(a, b, preferred_element_type=F32)


def encode(packed):
    peak = jnp.max(jnp.abs(packed), axis=0, keepdims=True)
    peak = jnp.maximum(peak, 1e-30)
    code = jnp.floor(packed * (TOP / peak) + 0.5).astype(jnp.int16)
    return code, jnp.broadcast_to(peak * (1.0 / TOP), (8, LANES))


def iota(shape, axis):
    return lax.broadcasted_iota(jnp.int32, shape, axis)


def weight(fine_index, coarse_index, coarse):
    nearest = jnp.right_shift(fine_index, 1)
    farther = nearest + 2 * jnp.bitwise_and(fine_index, 1) - 1
    value = jnp.where(coarse_index == nearest, 0.75, jnp.where(coarse_index == farther, 0.25, 0.0))
    return jnp.where((coarse_index >= 0) & (coarse_index < coarse), value, 0.0).astype(BF16)


def slope(ahead, behind):
    return jnp.where(ahead, 0.5, jnp.where(behind, -0.5, 0.0)).astype(BF16)


def blur(gap):
    value = jnp.where(gap == 1, 0.25, jnp.where(gap == 2, 0.0625, 0.0))
    return jnp.where(gap == 0, 0.375, value).astype(BF16)


def make_tables(up_x, up_y, slope_x, slope_y, blur_x, blur_y):
    finest = up_y.shape[0]
    coarse = blur_x.shape[0]
    piece = LANES - coarse
    shape = (LANES, finest)
    lane, column = iota(shape, 0), iota(shape, 1)
    up_x[0] = weight(column, lane, coarse)
    for j in range(up_x.shape[0] - 1):
        index = jnp.where(lane >= coarse, lane - coarse + piece * j, -1)
        up_x[1 + j] = weight(column, index, coarse)
    shape = up_y.shape
    row, column = iota(shape, 0), iota(shape, 1)
    up_y[...] = weight(row, jnp.where(column >= coarse, column - coarse, column), coarse)
    slope_y[...] = slope(column == row + 1, column == row - 1)
    slope_x[...] = slope(row == column + 1, row == column - 1)
    shape = blur_x.shape
    blur_x[...] = jnp.where(
        iota(shape, 1) < coarse, blur(jnp.abs(iota(shape, 0) - iota(shape, 1))), 0.0
    ).astype(BF16)
    shape = blur_y.shape
    column = iota(shape, 1)
    column = jnp.where(column >= coarse, column - coarse, column)
    blur_y[...] = blur(jnp.abs(iota(shape, 0) - column))


def fused_kernel(
    assign, images, momenta,
    codes, scales,
    up_x, up_y, slope_x, slope_y, blur_x, blur_y,
    ext, img, vel, fine, part, peer, ycode, yscale, mcode, mscale, xcode, xscale,
    lsem, hsend, hrecv, vsend, vrecv, psend, precv, ysend, yrecv,
    gsend, grecv, xsend, xrecv, osem, zsend, zrecv,
):
    level = lax.axis_index("level")
    group = lax.axis_index("subj")
    zone = lax.axis_index("gz")
    groups = lax.axis_size("subj")
    zones = lax.axis_size("gz")
    chips = groups // 2
    chip = group // 2
    core = group % 2
    partner = 2 * chip + 1 - core
    up = level
    fine_slab, finest = images.shape[1], images.shape[2]
    slab, coarse = momenta.shape[1], momenta.shape[3]
    rows_half, planes_half = slab // 2, fine_slab // 2
    pairs = (rows_half + 2) // 2
    rows_block, planes_block = rows_half // 2, planes_half // 2
    half = finest // 2
    rest = finest - LANES
    piece = LANES - coarse

    to_zone = zone + 1 - 2 * level
    has_to = (to_zone >= 0) & (to_zone < zones)
    from_zone = zone - 1 + 2 * level
    has_from = (from_zone >= 0) & (from_zone < zones)
    me = (level, group, zone)
    mate = (level, partner, zone)
    across = (1 - level, group, zone)
    upper = (level, group, to_zone)
    peers = [(chip + d) % chips for d in range(1, chips)]

    def remote(src, dst, send, recv, device):
        return pltpu.make_async_remote_copy(
            src_ref=src, dst_ref=dst, send_sem=send, recv_sem=recv,
            device_id=device, device_id_type=pl.DeviceIdType.MESH,
        )

    load_mom = pltpu.make_async_copy(
        momenta.at[:, pl.ds(level * (rows_half - 3), rows_half + 3)],
        ext.at[:, pl.ds(3 - 3 * level, rows_half + 3)],
        lsem.at[0],
    )
    load_img = pltpu.make_async_copy(
        images.at[:, pl.ds(level * (planes_half - 1), planes_half + 1)],
        img.at[:, pl.ds(1 - level, planes_half + 1)],
        lsem.at[1],
    )
    load_mom.start()
    load_img.start()
    barrier = pltpu.get_barrier_semaphore()

    def greet(device):
        pl.semaphore_signal(
            barrier, inc=1, device_id=device, device_id_type=pl.DeviceIdType.MESH
        )

    block = [(a, 2 * chip + b) for a in range(2) for b in range(2)]
    for a, b in block:
        @pl.when((a != level) | (b != group))
        def _(a=a, b=b):
            greet((a, b, zone))

    for other in peers:
        greet((level, 2 * other + core, zone))
    has_before = zone > 0
    has_after = zone < zones - 1

    @pl.when(has_before)
    def _():
        for a, b in block:
            greet((a, b, zone - 1))

    @pl.when(has_after)
    def _():
        for a, b in block:
            greet((a, b, zone + 1))

    make_tables(up_x, up_y, slope_x, slope_y, blur_x, blur_y)
    pl.semaphore_wait(
        barrier,
        3 + len(peers)
        + 4 * has_before.astype(jnp.int32) + 4 * has_after.astype(jnp.int32),
    )

    halo_mom = remote(
        momenta.at[:, pl.ds((1 - level) * (slab - 3), 3)],
        ext.at[:, pl.ds(level * (rows_half + 3), 3)],
        hsend.at[0], hrecv.at[0], upper,
    )
    halo_img = remote(
        images.at[:, pl.ds((1 - level) * (fine_slab - 1), 1)],
        img.at[:, pl.ds(level * (planes_half + 1), 1)],
        hsend.at[1], hrecv.at[1], upper,
    )

    @pl.when(has_to)
    def _():
        halo_mom.start()
        halo_img.start()

    @pl.when(jnp.logical_not(has_from))
    def _():
        for s in range(2):
            for e in range(3):
                for k in range(3):
                    ext[s, level * (rows_half + 3) + e, k] = jnp.zeros((coarse, coarse), F32)
            img[s, level * (planes_half + 1)] = jnp.zeros((finest, finest), BF16)

    load_mom.wait()

    def pair_of(i):
        return i + (1 - up) * (pairs - 1 - 2 * i)

    lane = lax.broadcasted_iota(jnp.int32, (coarse, LANES), 1)

    def velocity_sends(t):
        sends = [
            remote(
                vel.at[t, group], vel.at[t, group], vsend.at[t, 0], vrecv.at[t, group], mate
            )
        ]
        for n, other in enumerate(peers):
            sends.append(
                remote(
                    vel.at[t, group], vel.at[t, group], vsend.at[t, 1 + n],
                    vrecv.at[t, group], (level, 2 * other + core, zone),
                )
            )
        return sends

    def relay_sends(t):
        sends = []
        for n, other in enumerate(peers):
            there = 2 * other + core
            sends.append(
                remote(
                    vel.at[t, there], vel.at[t, there], vsend.at[t, chips + n],
                    vrecv.at[t, there], mate,
                )
            )
        return sends

    def smooth(i):
        t = pair_of(i)
        planes = {}
        for r in range(2):
            row = zone * slab + level * rows_half - 1 + 2 * t + r
            keep = ((row >= 0) & (row < slab * zones)).astype(F32)
            for s in range(2):
                for k in range(3):
                    f = [ext[s, 2 * t + r + o, k] for o in range(5)]
                    value = (f[0] + f[4]) * 0.0625 + (f[1] + f[3]) * 0.25 + f[2] * 0.375
                    wide = dot(split(value), blur_x[...])
                    wide = (wide[:coarse] + wide[coarse:]) * keep
                    planes[6 * r + 3 * s + k] = dot(blur_y[...], split(wide))
        for m in range(3):
            for j in range(3):
                turned = pltpu.roll(planes[9 + m], coarse - piece * j, 1)
                joined = jnp.where(lane < coarse, planes[3 * m + j], turned)
                vel[t, group, 3 * m + j] = joined.astype(BF16)

    def share(i):
        for send in velocity_sends(pair_of(i)):
            send.start()

    def begin(i, _):
        smooth(i)

        @pl.when(i > 0)
        def _():
            share(i - 1)

        return 0

    lax.fori_loop(0, pairs - 2, begin, 0)
    share(pairs - 3)

    load_img.wait()

    def relay(t):
        for send in relay_sends(t):
            send.wait_recv()
            send.start()

    def pick(t, source, first, count):
        value = vel[t, 0, first : first + count]
        for other in range(1, groups):
            value = jnp.where(source[other], vel[t, other, first : first + count], value)
        return value

    def raise_row(t, r, s, source):
        slot = lax.rem(2 * t + r, 4)
        if 6 * r + 3 * s < 9:
            chosen = pick(t, source, 6 * r + 3 * s, 3).reshape(3 * coarse, LANES)
            wide = dot(chosen, up_x[0])
            parts = [wide[coarse * k : coarse * (k + 1)] for k in range(3)]
        else:
            chosen = pick(t, source, 0, 9)
            parts = []
            for k in range(3):
                total = dot(chosen[3 * k], up_x[1])
                for j in range(1, 3):
                    total = total + dot(chosen[3 * k + j], up_x[1 + j])
                parts.append(total)
        for k in range(3):
            fine[s, slot, k] = dot(up_y[...], split(parts[k]))

    chunk = finest // 4

    def warp_plane(row, z):
        middle = lax.rem(row, 4)
        outer = lax.rem(row + 3 + 2 * z, 4)
        plane = 2 * (row - 1) + z
        for r in range(0, finest, chunk):
            rows = pl.ds(r, chunk)
            total = None
            for s in range(2):
                image = img[s, plane + 1, rows, :]
                dx = dot(image, slope_x[...])
                dy = dot(slope_y[rows, :], img[s, plane + 1])
                back = img[s, plane, rows, :].astype(F32)
                ahead = img[s, plane + 2, rows, :].astype(F32)
                dz = (ahead - back) * 0.5
                near = (
                    fine[s, middle, 0, rows, :] * dx
                    + fine[s, middle, 1, rows, :] * dy
                    + fine[s, middle, 2, rows, :] * dz
                )
                side = (
                    fine[s, outer, 0, rows, :] * dx
                    + fine[s, outer, 1, rows, :] * dy
                    + fine[s, outer, 2, rows, :] * dz
                )
                value = image.astype(F32) - (0.75 * near + 0.25 * side)
                total = value if total is None else total + value
            part[plane, rows, :] = total[:, :LANES]
            place = rest * (r // half)
            part[plane, pl.ds(finest + r % half, chunk), place : place + rest] = total[:, LANES:]

    def chip_send(row):
        here = lax.rem(row, rows_block)
        return remote(
            part.at[pl.ds(2 * row, 2)], peer.at[pl.ds(2 * here, 2)],
            psend.at[here], precv.at[here], mate,
        )

    def sum_sends(here):
        sends = []
        for n, other in enumerate(peers):
            there = (level, 2 * other + core, zone)
            at = pl.ds(2 * here, 2)
            sends.append(
                remote(
                    ycode.at[chip, at], ycode.at[chip, at], ysend.at[0, here, n],
                    yrecv.at[0, here, chip], there,
                )
            )
            sends.append(
                remote(
                    yscale.at[chip, at], yscale.at[chip, at], ysend.at[1, here, n],
                    yrecv.at[1, here, chip], there,
                )
            )
        return sends

    def settle(row):
        here = lax.rem(row, rows_block)
        chip_send(row).wait_recv()
        for z in range(2):
            code, scale = encode(part[2 * row + z] + peer[2 * here + z])
            ycode[chip, 2 * here + z] = code
            yscale[chip, 2 * here + z] = scale
        for send in sum_sends(here):
            send.start()

    def row_at(n):
        return n + (1 - up) * (rows_half - 1 - 2 * n)

    def owned(row):
        return (row // rows_block) == core

    subjects = 2 * groups
    base = 2 + (2 * level + core) * planes_block
    away = 2 + (2 * (1 - level) + core) * planes_block

    def block_row(n):
        return n + (1 - up) * (rows_block - 1 - 2 * n)

    def spread(here):
        at = pl.ds(2 * here, 2)
        out = pl.ds(base + 2 * here, 2)
        sends = []
        for n, (src, cross, dst) in enumerate(((mcode, xcode, codes), (mscale, xscale, scales))):
            sends += [
                remote(src.at[at], cross.at[at], xsend.at[n, here], xrecv.at[n, here], across),
                remote(src.at[at], dst.at[out], gsend.at[n, 0, here], grecv.at[n, 0, here], mate),
                pltpu.make_async_copy(src.at[at], dst.at[out], osem.at[n, 0, here]),
            ]
        return sends

    def hand_on(here):
        at = pl.ds(2 * here, 2)
        out = pl.ds(away + 2 * here, 2)
        sends = []
        for n, (src, dst) in enumerate(((xcode, codes), (xscale, scales))):
            sends += [
                remote(src.at[at], dst.at[out], gsend.at[n, 1, here], grecv.at[n, 1, here], mate),
                pltpu.make_async_copy(src.at[at], dst.at[out], osem.at[n, 1, here]),
            ]
        return sends

    outermost = (level == core) & has_from
    edge_at = pl.ds(level * 2 * (rows_block - 1), 2)
    edge_out = pl.ds((1 - level) * (fine_slab + 2), 2)

    def edge_sends():
        sends = []
        for m, (a, b) in enumerate(block):
            for n, (src, dst) in enumerate(((mcode, codes), (mscale, scales))):
                sends.append(
                    remote(
                        src.at[edge_at], dst.at[edge_out], zsend.at[n, m],
                        zrecv.at[n, 1 - level], (a, b, from_zone),
                    )
                )
        return sends

    def publish(here):
        at = pl.ds(2 * here, 2)
        for other in peers:
            for n, buffer in enumerate((ycode, yscale)):
                remote(
                    buffer.at[other, at], buffer.at[other, at], ysend.at[n, here, 0],
                    yrecv.at[n, here, other], me,
                ).wait_recv()
        for z in range(2):
            plane = 2 * here + z
            value = ycode[0, plane].astype(F32) * yscale[0, plane][:1]
            for other in range(1, chips):
                value = value + ycode[other, plane].astype(F32) * yscale[other, plane][:1]
            code, scale = encode(value * (1.0 / subjects))
            mcode[plane] = code
            mscale[plane] = scale
        for send in spread(here):
            send.start()

    is_first = core == 1 - up
    early = min(4, rows_block)
    halo_at = (pairs - 3) // 2
    sources = []
    for s in range(2):
        row = assign[2 * group + s]
        sources.append([row == 2 * other + s for other in range(groups)])

    relay(pair_of(0))

    def main(i, _):
        t = pair_of(i)

        @pl.when((i == halo_at) & has_from)
        def _():
            halo_mom.wait_recv()

        late = (i == halo_at) | (i == halo_at + 1)
        late_pair = pairs - 2 + i - halo_at

        @pl.when(late)
        def _():
            smooth(late_pair)

        for other in range(chips):
            theirs = 2 * other + 1 - core
            remote(
                vel.at[t, theirs], vel.at[t, theirs], vsend.at[t, 0], vrecv.at[t, theirs], mate
            ).wait_recv()
        for r in range(2):
            for s in range(2):
                raise_row(t, r, s, sources[s])

        @pl.when(late)
        def _():
            share(late_pair)

        @pl.when(i < pairs - 1)
        def _():
            relay(pair_of(i + 1))

        @pl.when((i == pairs - 1) & has_from)
        def _():
            halo_img.wait_recv()

        @pl.when(i >= 1)
        def _():
            def step(w, _):
                n = 2 * (i - 1) + w // 2
                row = row_at(n)
                warp_plane(row + 1, lax.rem(w, 2))

                @pl.when(lax.rem(w, 2) == 1)
                def _():
                    @pl.when(jnp.logical_not(owned(row)))
                    def _():
                        chip_send(row).start()

                    prior = row_at(jnp.maximum(n - 1, 0))

                    @pl.when((n > 0) & owned(prior))
                    def _():
                        settle(prior)

                @pl.when((i == pairs - 1) & is_first & (w < early))
                def _():
                    publish(block_row(w))

                return 0

            lax.fori_loop(0, 4, step, 0)

        return 0

    lax.fori_loop(0, pairs, main, 0)

    @pl.when(jnp.logical_not(is_first))
    def _():
        settle(row_at(rows_half - 1))

    def finish(n, _):
        @pl.when(jnp.logical_not(is_first) | (n >= early))
        def _():
            publish(block_row(n))

        return 0

    lax.fori_loop(0, rows_block, finish, 0)

    @pl.when(outermost)
    def _():
        for send in edge_sends():
            send.start()

    def hand(n, _):
        here = rows_block - 1 - block_row(n)
        first, second = spread(here)[0], spread(here)[3]
        first.wait_recv()
        second.wait_recv()
        for send in hand_on(here):
            send.start()
        return 0

    lax.fori_loop(0, rows_block, hand, 0)

    @pl.when(has_to)
    def _():
        halo_mom.wait_send()
        halo_img.wait_send()

    def drain_velocity(t, _):
        for send in velocity_sends(t) + relay_sends(t):
            send.wait_send()
        return 0

    lax.fori_loop(0, pairs, drain_velocity, 0)

    def drain_rows(here, _):
        chip_send((1 - core) * rows_block + here).wait_send()
        for send in sum_sends(here):
            send.wait_send()
        for n, send in enumerate(spread(here)):
            if n % 3 == 0:
                send.wait_send()
            else:
                send.wait()
        for send in hand_on(here):
            send.wait()
        return 0

    lax.fori_loop(0, rows_block, drain_rows, 0)

    @pl.when(outermost)
    def _():
        for send in edge_sends():
            send.wait_send()

    for side, there in ((0, has_before), (1, has_after)):
        @pl.when(there)
        def _(side=side):
            out = pl.ds(side * (fine_slab + 2), 2)
            for n, dst in enumerate((codes, scales)):
                remote(dst.at[out], dst.at[out], zsend.at[n, 0], zrecv.at[n, side], me).wait_recv()


def fused(assign, images, momenta):
    groups = lax.axis_size("subj")
    chips = groups // 2
    fine_slab, finest = images.shape[1], images.shape[2]
    slab, coarse = momenta.shape[1], momenta.shape[3]
    rows_half, planes_half = slab // 2, fine_slab // 2
    pairs = (rows_half + 2) // 2
    rows_block, planes_block = rows_half // 2, planes_half // 2
    tall = finest + finest // 2
    tables = 1 + coarse // (LANES - coarse)
    dma = pltpu.SemaphoreType.DMA
    hbm = pl.BlockSpec(memory_space=pl.ANY)
    scratch = [
        pltpu.VMEM((tables, LANES, finest), BF16),
        pltpu.VMEM((finest, finest), BF16),
        pltpu.VMEM((finest, finest), BF16),
        pltpu.VMEM((finest, finest), BF16),
        pltpu.VMEM((coarse, LANES), BF16),
        pltpu.VMEM((coarse, 2 * coarse), BF16),
        pltpu.VMEM((2, rows_half + 6, 3, coarse, coarse), F32),
        pltpu.VMEM((2, planes_half + 2, finest, finest), BF16),
        pltpu.VMEM((pairs, groups, 9, coarse, LANES), BF16),
        pltpu.VMEM((2, 4, 3, finest, finest), F32),
        pltpu.VMEM((planes_half, tall, LANES), F32),
        pltpu.VMEM((planes_block, tall, LANES), F32),
        pltpu.VMEM((chips, planes_block, tall, LANES), jnp.int16),
        pltpu.VMEM((chips, planes_block, 8, LANES), F32),
        pltpu.VMEM((planes_block, tall, LANES), jnp.int16),
        pltpu.VMEM((planes_block, 8, LANES), F32),
        pltpu.VMEM((planes_block, tall, LANES), jnp.int16),
        pltpu.VMEM((planes_block, 8, LANES), F32),
        dma((2,)),
        dma((2,)),
        dma((2,)),
        dma((pairs, 2 * chips)),
        dma((pairs, groups)),
        dma((rows_block,)),
        dma((rows_block,)),
        dma((2, rows_block, max(chips - 1, 1))),
        dma((2, rows_block, chips)),
        dma((2, 2, rows_block)),
        dma((2, 2, rows_block)),
        dma((2, rows_block)),
        dma((2, rows_block)),
        dma((2, 2, rows_block)),
        dma((2, 4)),
        dma((2, 2)),
    ]
    return pl.pallas_call(
        fused_kernel,
        out_shape=(
            jax.ShapeDtypeStruct((fine_slab + 4, tall, LANES), jnp.int16),
            jax.ShapeDtypeStruct((fine_slab + 4, 8, LANES), F32),
        ),
        in_specs=[pl.BlockSpec(memory_space=pltpu.SMEM), hbm, hbm],
        out_specs=(hbm, hbm),
        scratch_shapes=scratch,
        compiler_params=pltpu.CompilerParams(
            collective_id=0, has_side_effects=True, vmem_limit_bytes=60 * 1024 * 1024
        ),
    )(assign, images, momenta)


STEP = 4
RING = 8


def sweep_kernel(codes, scales, out, first, second):
    step = pl.program_id(0)
    last = pl.num_programs(0) - 1
    zone = lax.axis_index("gz")
    zones = lax.axis_size("gz")
    finest = out.shape[1]
    half = finest // 2
    rest = finest - LANES
    wide_at = MARGIN
    tail_at = finest + 3 * MARGIN
    base = STEP * lax.rem(step, 2)
    lane = iota((half, LANES), 1)
    edge = iota((MARGIN, LANES), 1)
    low = zone == 0
    high = zone == zones - 1

    def slot(o):
        return lax.rem(base + o + RING, RING)

    def put(ref, at, top, bottom, tail):
        ref[at, pl.ds(wide_at, half), :] = top
        ref[at, pl.ds(wide_at + half, half), :] = bottom
        ref[at, pl.ds(tail_at, half), :] = tail
        above = pltpu.roll(tail[half - MARGIN :], LANES - rest, 1)
        below = pltpu.roll(tail[:MARGIN], LANES - rest, 1)
        ref[at, pl.ds(tail_at - MARGIN, MARGIN), :] = jnp.where(edge >= rest, above, 0.0)
        ref[at, pl.ds(tail_at + half, MARGIN), :] = jnp.where(edge < rest, below, 0.0)

    def around(ref, o, at, center):
        rows = pl.ds(at, half)
        here = slot(o)
        return (
            ref[slot(o - 1), rows, :]
            + ref[slot(o + 1), rows, :]
            + ref[here, pl.ds(at - 1, half), :]
            + ref[here, pl.ds(at + 1, half), :]
        )

    def relax(ref, o):
        here = slot(o)
        top = ref[here, pl.ds(wide_at, half), :]
        bottom = ref[here, pl.ds(wide_at + half, half), :]
        tail = ref[here, pl.ds(tail_at, half), :]
        top_west = pltpu.roll(top, 1, 1)
        bottom_west = pltpu.roll(bottom, 1, 1)
        tail_east = pltpu.roll(tail, LANES - 1, 1)
        total = around(ref, o, wide_at, top)
        total = total + jnp.where(lane == 0, 0.0, top_west)
        total = total + jnp.where(lane == LANES - 1, tail_east, pltpu.roll(top, LANES - 1, 1))
        new_top = 0.1 * top + 0.15 * total
        total = around(ref, o, wide_at + half, bottom)
        total = total + jnp.where(lane == 0, 0.0, bottom_west)
        total = total + jnp.where(
            lane == LANES - 1, pltpu.roll(tail, rest - 1, 1), pltpu.roll(bottom, LANES - 1, 1)
        )
        new_bottom = 0.1 * bottom + 0.15 * total
        total = around(ref, o, tail_at, tail)
        west = jnp.where(lane == 0, top_west, pltpu.roll(tail, 1, 1))
        total = total + jnp.where(lane == rest, pltpu.roll(bottom, rest + 1, 1), west)
        ends = (lane == rest - 1) | (lane == LANES - 1)
        total = total + jnp.where(ends, 0.0, tail_east)
        new_tail = 0.1 * tail + 0.15 * total
        return new_top, new_bottom, new_tail

    @pl.when(step == 0)
    def _():
        first[...] = jnp.zeros_like(first)
        second[...] = jnp.zeros_like(second)

    for o in range(STEP):
        value = codes[o].astype(F32) * scales[o][:1]
        if o < 2:
            value = jnp.where((step == 0) & low, 0.0, value)
        else:
            value = jnp.where((step == last) & high, 0.0, value)
        put(first, slot(o), value[:half], value[half:finest], value[finest:])

    for o in range(-1, STEP - 1):
        parts = relax(first, o)
        if o == 1:
            parts = [jnp.where((step == 0) & low, 0.0, p) for p in parts]
        if o == 2:
            parts = [jnp.where((step == last) & high, 0.0, p) for p in parts]
        put(second, slot(o), *parts)

    @pl.when(step >= 1)
    def _():
        for o in range(-2, STEP - 2):
            top, bottom, tail = relax(second, o)
            out[o + 2, 0:half, 0:LANES] = top
            out[o + 2, half:finest, 0:LANES] = bottom
            out[o + 2, 0:half, LANES:finest] = tail[:, :rest]
            out[o + 2, half:finest, LANES:finest] = pltpu.roll(tail, rest, 1)[:, :rest]


def sweeps(codes, scales, finest):
    planes, tall = codes.shape[0] - 4, codes.shape[1]
    ring = pltpu.VMEM((RING, tall + 4 * MARGIN, LANES), F32)
    return pl.pallas_call(
        sweep_kernel,
        grid=(planes // STEP + 1,),
        in_specs=[
            pl.BlockSpec((STEP, tall, LANES), lambda j: (j, 0, 0)),
            pl.BlockSpec((STEP, 8, LANES), lambda j: (j, 0, 0)),
        ],
        out_specs=pl.BlockSpec(
            (STEP, finest, finest), lambda j: (jnp.maximum(j - 1, 0), 0, 0)
        ),
        out_shape=jax.ShapeDtypeStruct((planes, finest, finest), F32),
        scratch_shapes=[ring, ring],
        compiler_params=pltpu.CompilerParams(dimension_semantics=("arbitrary",)),
    )(codes, scales)


def shards(images, momenta, assign):
    codes, scales = fused(assign, images, momenta)
    return sweeps(codes, scales, images.shape[2])


def solution(mesh):
    return jax.shard_map(
        shards,
        mesh=mesh,
        in_specs=(P("subj", "gz", None, None), P("subj", "gz", None, None, None), P()),
        out_specs=P("gz", None, None),
        check_vma=False,
    )
```

```python
import functools

import jax
import jax.numpy as jnp
from jax import lax
from jax.experimental import pallas as pl
from jax.experimental.pallas import tpu as pltpu
from jax.sharding import PartitionSpec as P

LANES = 128
MARGIN = 8
TOP = 32767.0
LIMIT = 18.0
F32 = jnp.float32
BF16 = jnp.bfloat16


def split(value):
    high = value.astype(BF16)
    low = (value - high.astype(F32)).astype(BF16)
    return jnp.concatenate([high, low], axis=0)


def dot(a, b):
    return jnp.dot(a, b, preferred_element_type=F32)


def encode(packed):
    peak = jnp.max(jnp.abs(packed), axis=0, keepdims=True)
    peak = jnp.maximum(peak, 1e-30)
    code = jnp.floor(packed * (TOP / peak) + 0.5).astype(jnp.int16)
    return code, jnp.broadcast_to(peak * (1.0 / TOP), (8, LANES))


def iota(shape, axis):
    return lax.broadcasted_iota(jnp.int32, shape, axis)


def weight(fine_index, coarse_index, coarse):
    nearest = jnp.right_shift(fine_index, 1)
    farther = nearest + 2 * jnp.bitwise_and(fine_index, 1) - 1
    value = jnp.where(coarse_index == nearest, 0.75, jnp.where(coarse_index == farther, 0.25, 0.0))
    return jnp.where((coarse_index >= 0) & (coarse_index < coarse), value, 0.0).astype(BF16)


def slope(ahead, behind):
    return jnp.where(ahead, 0.5, jnp.where(behind, -0.5, 0.0)).astype(BF16)


def blur(gap):
    value = jnp.where(gap == 1, 0.25, jnp.where(gap == 2, 0.0625, 0.0))
    return jnp.where(gap == 0, 0.375, value).astype(BF16)


def make_tables(up_x, up_y, slope_x, slope_y, blur_x, blur_y):
    finest = up_y.shape[0]
    coarse = blur_x.shape[0]
    piece = LANES - coarse
    shape = (LANES, finest)
    lane, column = iota(shape, 0), iota(shape, 1)
    up_x[0] = weight(column, lane, coarse)
    for j in range(up_x.shape[0] - 1):
        index = jnp.where(lane >= coarse, lane - coarse + piece * j, -1)
        up_x[1 + j] = weight(column, index, coarse)
    shape = up_y.shape
    row, column = iota(shape, 0), iota(shape, 1)
    up_y[...] = weight(row, jnp.where(column >= coarse, column - coarse, column), coarse)
    slope_y[...] = slope(column == row + 1, column == row - 1)
    slope_x[...] = slope(row == column + 1, row == column - 1)
    shape = blur_x.shape
    blur_x[...] = jnp.where(
        iota(shape, 1) < coarse, blur(jnp.abs(iota(shape, 0) - iota(shape, 1))), 0.0
    ).astype(BF16)
    shape = blur_y.shape
    column = iota(shape, 1)
    column = jnp.where(column >= coarse, column - coarse, column)
    blur_y[...] = blur(jnp.abs(iota(shape, 0) - column))


def fused_kernel(
    messages, assign, images, momenta,
    codes, scales,
    up_x, up_y, slope_x, slope_y, blur_x, blur_y,
    ext, edges, hout, hin, img, vel, ymsg, fine, part, peer, ycode, yscale, mcode, mscale, xcode, xscale,
    lsem, hsend, hrecv, vsend, vrecv, qsend, qrecv, psend, precv, ysend, yrecv,
    gsend, grecv, xsend, xrecv, osem, zsend, zrecv,
):
    level = lax.axis_index("level")
    group = lax.axis_index("subj")
    zone = lax.axis_index("gz")
    groups = lax.axis_size("subj")
    zones = lax.axis_size("gz")
    chips = groups // 2
    chip = group // 2
    core = group % 2
    partner = 2 * chip + 1 - core
    up = level
    fine_slab, finest = images.shape[1], images.shape[2]
    slab, coarse = momenta.shape[1], momenta.shape[3]
    rows_half, planes_half = slab // 2, fine_slab // 2
    pairs = (rows_half + 2) // 2
    rows_block, planes_block = rows_half // 2, planes_half // 2
    half = finest // 2
    rest = finest - LANES
    piece = LANES - coarse

    to_zone = zone + 1 - 2 * level
    has_to = (to_zone >= 0) & (to_zone < zones)
    from_zone = zone - 1 + 2 * level
    has_from = (from_zone >= 0) & (from_zone < zones)
    me = (level, group, zone)
    mate = (level, partner, zone)
    across = (1 - level, group, zone)
    upper = (level, group, to_zone)
    peers = [(chip + d) % chips for d in range(1, chips)]

    def remote(src, dst, send, recv, device):
        return pltpu.make_async_remote_copy(
            src_ref=src, dst_ref=dst, send_sem=send, recv_sem=recv,
            device_id=device, device_id_type=pl.DeviceIdType.MESH,
        )

    load_mom = pltpu.make_async_copy(
        momenta.at[:, pl.ds(level * (rows_half - 3), rows_half + 3)],
        ext.at[:, pl.ds(3 - 3 * level, rows_half + 3)],
        lsem.at[0],
    )
    load_img = pltpu.make_async_copy(
        images.at[:, pl.ds(level * (planes_half - 1), planes_half + 1)],
        img.at[:, pl.ds(1 - level, planes_half + 1)],
        lsem.at[1],
    )
    load_edges = pltpu.make_async_copy(
        momenta.at[:, pl.ds((1 - level) * (slab - 3), 3)], edges, lsem.at[2]
    )
    load_edges.start()
    load_mom.start()
    barrier = pltpu.get_barrier_semaphore()

    def greet(device):
        pl.semaphore_signal(
            barrier, inc=1, device_id=device, device_id_type=pl.DeviceIdType.MESH
        )

    block = [(a, 2 * chip + b) for a in range(2) for b in range(2)]
    for a, b in block:
        @pl.when((a != level) | (b != group))
        def _(a=a, b=b):
            greet((a, b, zone))

    for other in peers:
        greet((level, 2 * other + core, zone))
    has_before = zone > 0
    has_after = zone < zones - 1

    @pl.when(has_before)
    def _():
        for a, b in block:
            greet((a, b, zone - 1))

    @pl.when(has_after)
    def _():
        for a, b in block:
            greet((a, b, zone + 1))

    make_tables(up_x, up_y, slope_x, slope_y, blur_x, blur_y)
    load_edges.wait()
    for s in range(2):
        for e in range(3):
            for k in range(3):
                code = jnp.floor(edges[s, e, k] * (TOP / LIMIT) + 0.5)
                hout[s, e, k] = jnp.clip(code, -TOP, TOP).astype(jnp.int16)
    pl.semaphore_wait(
        barrier,
        3 + len(peers)
        + 4 * has_before.astype(jnp.int32) + 4 * has_after.astype(jnp.int32),
    )

    halo_mom = remote(hout, hin, hsend.at[0], hrecv.at[0], upper)
    halo_img = remote(
        images.at[:, pl.ds((1 - level) * (fine_slab - 1), 1)],
        img.at[:, pl.ds(level * (planes_half + 1), 1)],
        hsend.at[1], hrecv.at[1], upper,
    )

    @pl.when(has_to)
    def _():
        halo_mom.start()
        halo_img.start()

    @pl.when(jnp.logical_not(has_from))
    def _():
        for s in range(2):
            for e in range(3):
                for k in range(3):
                    ext[s, level * (rows_half + 3) + e, k] = jnp.zeros((coarse, coarse), F32)
            img[s, level * (planes_half + 1)] = jnp.zeros((finest, finest), BF16)

    load_mom.wait()
    load_img.start()

    def pair_of(i):
        return i + (1 - up) * (pairs - 1 - 2 * i)

    strip = coarse // 2
    lane = iota((strip, LANES), 1)

    sources = [assign[2 * group + s] for s in range(2)]
    pieces = [(s, c) for s in range(2) for c in range(2)]

    def ranks(home):
        count = jnp.int32(0)
        places = {}
        for s, c in pieces:
            needed = jnp.bool_(False)
            for d in range(1, chips):
                there = (home + d) % chips
                for b in range(2):
                    row = assign[2 * (2 * there + b) + s]
                    needed = needed | (row == 2 * (2 * home + c) + s)
            places[s, c] = (needed, count)
            count = count + needed.astype(jnp.int32)
        return places

    def near_flag(s, c):
        return sources[s] == 2 * (2 * chip + c) + s

    if messages == 1:
        mine = ranks(chip)
        theirs_of = {other: ranks(peer_chip) for other, peer_chip in enumerate(peers)}

    def item_flag(s, other, n):
        if messages == 2:
            if n // 2 != s:
                return None
            return sources[s] == 2 * (2 * peers[other] + n % 2) + s
        flag = jnp.bool_(False)
        for c in range(2):
            needed, place = theirs_of[other][s, c]
            here = sources[s] == 2 * (2 * peers[other] + c) + s
            flag = flag | (here & needed & (place == n))
        return flag

    def near_send(t):
        return remote(vel.at[t, core], vel.at[t, core], vsend.at[t], vrecv.at[t], mate)

    def message_sends(t):
        part_of = ymsg.at[t, chip, :, pl.ds(strip * core, strip)]
        return [
            remote(
                part_of, part_of, qsend.at[t, n], qrecv.at[t, chip, core],
                (level, 2 * other + core, zone),
            )
            for n, other in enumerate(peers)
        ]

    def relay_sends(t):
        sends = []
        for n, other in enumerate(peers):
            part_of = ymsg.at[t, other, :, pl.ds(strip * core, strip)]
            sends.append(
                remote(
                    part_of, part_of, qsend.at[t, chips - 1 + n], qrecv.at[t, other, core], mate
                )
            )
        return sends

    def await_relayed(t):
        for other in peers:
            part_of = ymsg.at[t, other, :, pl.ds(strip * (1 - core), strip)]
            remote(
                part_of, part_of, qsend.at[t, 0], qrecv.at[t, other, 1 - core], mate
            ).wait_recv()

    def smooth(i):
        t = pair_of(i)
        planes = {}
        for r in range(2):
            row = zone * slab + level * rows_half - 1 + 2 * t + r
            keep = ((row >= 0) & (row < slab * zones)).astype(F32)
            for s in range(2):
                for k in range(3):
                    f = [ext[s, 2 * t + r + o, k] for o in range(5)]
                    value = (f[0] + f[4]) * 0.0625 + (f[1] + f[3]) * 0.25 + f[2] * 0.375
                    wide = dot(split(value), blur_x[...])
                    wide = (wide[:coarse] + wide[coarse:]) * keep
                    planes[6 * r + 3 * s + k] = dot(blur_y[...], split(wide))
        for p in range(12):
            vel[t, core, p] = planes[p].astype(BF16)

    def compose(t):
        rows = pl.ds(strip * core, strip)
        for m in range(messages):
            planes = []
            for r in range(2):
                for n in (2 * m, 2 * m + 1):
                    for k in range(3):
                        if messages == 2:
                            value = vel[t, n % 2, 6 * r + 3 * (n // 2) + k, rows]
                        else:
                            value = vel[t, 0, 6 * r + k, rows]
                            for s, c in pieces[1:]:
                                needed, place = mine[s, c]
                                value = jnp.where(
                                    needed & (place == n),
                                    vel[t, c, 6 * r + 3 * s + k, rows],
                                    value,
                                )
                        planes.append(value)
            for a in range(3):
                extra = planes[9 + a].astype(F32)
                for j in range(3):
                    turned = pltpu.roll(extra, coarse - piece * j, 1)
                    joined = jnp.where(lane < coarse, planes[3 * a + j].astype(F32), turned)
                    ymsg[t, chip, 9 * m + 3 * a + j, rows] = joined.astype(BF16)

    def share(i):
        t = pair_of(i)
        near_send(t).wait_recv()
        compose(t)
        for send in message_sends(t):
            send.start()

    def begin(i, _):
        smooth(i)
        near_send(pair_of(i)).start()

        @pl.when(i > 0)
        def _():
            share(i - 1)

        return 0

    lax.fori_loop(0, pairs - 2, begin, 0)
    share(pairs - 3)

    load_img.wait()

    def relay(t):
        for send in relay_sends(t):
            send.wait_recv()
            send.start()

    def raise_row(t, r, s):
        slot = lax.rem(2 * t + r, 4)
        p = 6 * r + 3 * s
        value = jnp.where(near_flag(s, 1), vel[t, 1, p : p + 3], vel[t, 0, p : p + 3])
        spread_out, spread_flag = None, jnp.bool_(False)
        for other in range(len(peers)):
            for n in range(2 * messages):
                flag = item_flag(s, other, n)
                if flag is None:
                    continue
                first = 9 * (n // 2)
                if r == 0 or n % 2 == 0:
                    at = first + 6 * r + 3 * (n % 2)
                    value = jnp.where(flag, ymsg[t, peers[other], at : at + 3], value)
                else:
                    group_of = ymsg[t, peers[other], first : first + 9]
                    if spread_out is None:
                        spread_out = group_of
                    else:
                        spread_out = jnp.where(flag, group_of, spread_out)
                    spread_flag = spread_flag | flag
        wide = dot(value.reshape(3 * coarse, LANES), up_x[0])
        for k in range(3):
            part_of = wide[coarse * k : coarse * (k + 1)]
            if spread_out is not None:
                total = dot(spread_out[3 * k], up_x[1])
                for j in range(1, 3):
                    total = total + dot(spread_out[3 * k + j], up_x[1 + j])
                part_of = jnp.where(spread_flag, total, part_of)
            fine[s, slot, k] = dot(up_y[...], split(part_of))

    chunk = finest // 4

    def warp_plane(row, z):
        middle = lax.rem(row, 4)
        outer = lax.rem(row + 3 + 2 * z, 4)
        plane = 2 * (row - 1) + z
        for r in range(0, finest, chunk):
            rows = pl.ds(r, chunk)
            total = None
            for s in range(2):
                image = img[s, plane + 1, rows, :]
                dx = dot(image, slope_x[...])
                dy = dot(slope_y[rows, :], img[s, plane + 1])
                back = img[s, plane, rows, :].astype(F32)
                ahead = img[s, plane + 2, rows, :].astype(F32)
                dz = (ahead - back) * 0.5
                near = (
                    fine[s, middle, 0, rows, :] * dx
                    + fine[s, middle, 1, rows, :] * dy
                    + fine[s, middle, 2, rows, :] * dz
                )
                side = (
                    fine[s, outer, 0, rows, :] * dx
                    + fine[s, outer, 1, rows, :] * dy
                    + fine[s, outer, 2, rows, :] * dz
                )
                value = image.astype(F32) - (0.75 * near + 0.25 * side)
                total = value if total is None else total + value
            part[plane, rows, :] = total[:, :LANES]
            place = rest * (r // half)
            part[plane, pl.ds(finest + r % half, chunk), place : place + rest] = total[:, LANES:]

    def chip_send(row):
        here = lax.rem(row, rows_block)
        return remote(
            part.at[pl.ds(2 * row, 2)], peer.at[pl.ds(2 * here, 2)],
            psend.at[here], precv.at[here], mate,
        )

    def sum_sends(here):
        sends = []
        for n, other in enumerate(peers):
            there = (level, 2 * other + core, zone)
            at = pl.ds(2 * here, 2)
            sends.append(
                remote(
                    ycode.at[chip, at], ycode.at[chip, at], ysend.at[0, here, n],
                    yrecv.at[0, here, chip], there,
                )
            )
            sends.append(
                remote(
                    yscale.at[chip, at], yscale.at[chip, at], ysend.at[1, here, n],
                    yrecv.at[1, here, chip], there,
                )
            )
        return sends

    def settle(row):
        here = lax.rem(row, rows_block)
        chip_send(row).wait_recv()
        for z in range(2):
            code, scale = encode(part[2 * row + z] + peer[2 * here + z])
            ycode[chip, 2 * here + z] = code
            yscale[chip, 2 * here + z] = scale
        for send in sum_sends(here):
            send.start()

    def row_at(n):
        return n + (1 - up) * (rows_half - 1 - 2 * n)

    def owned(row):
        return (row // rows_block) == core

    subjects = 2 * groups
    base = 2 + (2 * level + core) * planes_block
    away = 2 + (2 * (1 - level) + core) * planes_block

    def block_row(n):
        return n + (1 - up) * (rows_block - 1 - 2 * n)

    def spread(here):
        at = pl.ds(2 * here, 2)
        out = pl.ds(base + 2 * here, 2)
        sends = []
        for n, (src, cross, dst) in enumerate(((mcode, xcode, codes), (mscale, xscale, scales))):
            sends += [
                remote(src.at[at], cross.at[at], xsend.at[n, here], xrecv.at[n, here], across),
                remote(src.at[at], dst.at[out], gsend.at[n, 0, here], grecv.at[n, 0, here], mate),
                pltpu.make_async_copy(src.at[at], dst.at[out], osem.at[n, 0, here]),
            ]
        return sends

    def hand_on(here):
        at = pl.ds(2 * here, 2)
        out = pl.ds(away + 2 * here, 2)
        sends = []
        for n, (src, dst) in enumerate(((xcode, codes), (xscale, scales))):
            sends += [
                remote(src.at[at], dst.at[out], gsend.at[n, 1, here], grecv.at[n, 1, here], mate),
                pltpu.make_async_copy(src.at[at], dst.at[out], osem.at[n, 1, here]),
            ]
        return sends

    outermost = (level == core) & has_from
    edge_at = pl.ds(level * 2 * (rows_block - 1), 2)
    edge_out = pl.ds((1 - level) * (fine_slab + 2), 2)

    def edge_sends():
        sends = []
        for m, (a, b) in enumerate(block):
            for n, (src, dst) in enumerate(((mcode, codes), (mscale, scales))):
                sends.append(
                    remote(
                        src.at[edge_at], dst.at[edge_out], zsend.at[n, m],
                        zrecv.at[n, 1 - level], (a, b, from_zone),
                    )
                )
        return sends

    def publish(here):
        at = pl.ds(2 * here, 2)
        for other in peers:
            for n, buffer in enumerate((ycode, yscale)):
                remote(
                    buffer.at[other, at], buffer.at[other, at], ysend.at[n, here, 0],
                    yrecv.at[n, here, other], me,
                ).wait_recv()
        for z in range(2):
            plane = 2 * here + z
            value = ycode[0, plane].astype(F32) * yscale[0, plane][:1]
            for other in range(1, chips):
                value = value + ycode[other, plane].astype(F32) * yscale[other, plane][:1]
            code, scale = encode(value * (1.0 / subjects))
            mcode[plane] = code
            mscale[plane] = scale
        for send in spread(here):
            send.start()

    is_first = core == 1 - up
    early = min(4, rows_block)
    halo_at = (pairs - 3) // 2
    relay(pair_of(0))

    def main(i, _):
        t = pair_of(i)

        @pl.when((i == halo_at) & has_from)
        def _():
            halo_mom.wait_recv()
            for s in range(2):
                for e in range(3):
                    for k in range(3):
                        value = hin[s, e, k].astype(F32) * (LIMIT / TOP)
                        ext[s, level * (rows_half + 3) + e, k] = value

        late = (i == halo_at) | (i == halo_at + 1)
        late_pair = pairs - 2 + i - halo_at

        @pl.when(late)
        def _():
            smooth(late_pair)
            near_send(pair_of(late_pair)).start()

        @pl.when(i < pairs - 1)
        def _():
            relay(pair_of(i + 1))

        await_relayed(t)
        for r in range(2):
            for s in range(2):
                raise_row(t, r, s)

        @pl.when(late)
        def _():
            share(late_pair)

        @pl.when((i == pairs - 1) & has_from)
        def _():
            halo_img.wait_recv()

        @pl.when(i >= 1)
        def _():
            def step(w, _):
                n = 2 * (i - 1) + w // 2
                row = row_at(n)
                warp_plane(row + 1, lax.rem(w, 2))

                @pl.when(lax.rem(w, 2) == 1)
                def _():
                    @pl.when(jnp.logical_not(owned(row)))
                    def _():
                        chip_send(row).start()

                    prior = row_at(jnp.maximum(n - 1, 0))

                    @pl.when((n > 0) & owned(prior))
                    def _():
                        settle(prior)

                @pl.when((i == pairs - 1) & is_first & (w < early))
                def _():
                    publish(block_row(w))

                return 0

            lax.fori_loop(0, 4, step, 0)

        return 0

    lax.fori_loop(0, pairs, main, 0)

    @pl.when(jnp.logical_not(is_first))
    def _():
        settle(row_at(rows_half - 1))

    def finish(n, _):
        @pl.when(jnp.logical_not(is_first) | (n >= early))
        def _():
            publish(block_row(n))

        return 0

    lax.fori_loop(0, rows_block, finish, 0)

    @pl.when(outermost)
    def _():
        for send in edge_sends():
            send.start()

    def hand(n, _):
        here = rows_block - 1 - block_row(n)
        first, second = spread(here)[0], spread(here)[3]
        first.wait_recv()
        second.wait_recv()
        for send in hand_on(here):
            send.start()
        return 0

    lax.fori_loop(0, rows_block, hand, 0)

    @pl.when(has_to)
    def _():
        halo_mom.wait_send()
        halo_img.wait_send()

    def drain_velocity(t, _):
        near_send(t).wait_send()
        for send in message_sends(t) + relay_sends(t):
            send.wait_send()
        return 0

    lax.fori_loop(0, pairs, drain_velocity, 0)

    def drain_rows(here, _):
        chip_send((1 - core) * rows_block + here).wait_send()
        for send in sum_sends(here):
            send.wait_send()
        for n, send in enumerate(spread(here)):
            if n % 3 == 0:
                send.wait_send()
            else:
                send.wait()
        for send in hand_on(here):
            send.wait()
        return 0

    lax.fori_loop(0, rows_block, drain_rows, 0)

    @pl.when(outermost)
    def _():
        for send in edge_sends():
            send.wait_send()

    for side, there in ((0, has_before), (1, has_after)):
        @pl.when(there)
        def _(side=side):
            out = pl.ds(side * (fine_slab + 2), 2)
            for n, dst in enumerate((codes, scales)):
                remote(dst.at[out], dst.at[out], zsend.at[n, 0], zrecv.at[n, side], me).wait_recv()


def fused(messages, assign, images, momenta):
    groups = lax.axis_size("subj")
    chips = groups // 2
    fine_slab, finest = images.shape[1], images.shape[2]
    slab, coarse = momenta.shape[1], momenta.shape[3]
    rows_half, planes_half = slab // 2, fine_slab // 2
    pairs = (rows_half + 2) // 2
    rows_block, planes_block = rows_half // 2, planes_half // 2
    tall = finest + finest // 2
    tables = 1 + coarse // (LANES - coarse)
    dma = pltpu.SemaphoreType.DMA
    hbm = pl.BlockSpec(memory_space=pl.ANY)
    scratch = [
        pltpu.VMEM((tables, LANES, finest), BF16),
        pltpu.VMEM((finest, finest), BF16),
        pltpu.VMEM((finest, finest), BF16),
        pltpu.VMEM((finest, finest), BF16),
        pltpu.VMEM((coarse, LANES), BF16),
        pltpu.VMEM((coarse, 2 * coarse), BF16),
        pltpu.VMEM((2, rows_half + 6, 3, coarse, coarse), F32),
        pltpu.VMEM((2, 3, 3, coarse, coarse), F32),
        pltpu.VMEM((2, 3, 3, coarse, coarse), jnp.int16),
        pltpu.VMEM((2, 3, 3, coarse, coarse), jnp.int16),
        pltpu.VMEM((2, planes_half + 2, finest, finest), BF16),
        pltpu.VMEM((pairs, 2, 12, coarse, LANES), BF16),
        pltpu.VMEM((pairs, chips, 9 * messages, coarse, LANES), BF16),
        pltpu.VMEM((2, 4, 3, finest, finest), F32),
        pltpu.VMEM((planes_half, tall, LANES), F32),
        pltpu.VMEM((planes_block, tall, LANES), F32),
        pltpu.VMEM((chips, planes_block, tall, LANES), jnp.int16),
        pltpu.VMEM((chips, planes_block, 8, LANES), F32),
        pltpu.VMEM((planes_block, tall, LANES), jnp.int16),
        pltpu.VMEM((planes_block, 8, LANES), F32),
        pltpu.VMEM((planes_block, tall, LANES), jnp.int16),
        pltpu.VMEM((planes_block, 8, LANES), F32),
        dma((3,)),
        dma((2,)),
        dma((2,)),
        dma((pairs,)),
        dma((pairs,)),
        dma((pairs, 2 * (chips - 1))),
        dma((pairs, chips, 2)),
        dma((rows_block,)),
        dma((rows_block,)),
        dma((2, rows_block, max(chips - 1, 1))),
        dma((2, rows_block, chips)),
        dma((2, 2, rows_block)),
        dma((2, 2, rows_block)),
        dma((2, rows_block)),
        dma((2, rows_block)),
        dma((2, 2, rows_block)),
        dma((2, 4)),
        dma((2, 2)),
    ]
    return pl.pallas_call(
        functools.partial(fused_kernel, messages),
        out_shape=(
            jax.ShapeDtypeStruct((fine_slab + 4, tall, LANES), jnp.int16),
            jax.ShapeDtypeStruct((fine_slab + 4, 8, LANES), F32),
        ),
        in_specs=[pl.BlockSpec(memory_space=pltpu.SMEM), hbm, hbm],
        out_specs=(hbm, hbm),
        scratch_shapes=scratch,
        compiler_params=pltpu.CompilerParams(
            collective_id=messages, has_side_effects=True, vmem_limit_bytes=60 * 1024 * 1024
        ),
    )(assign, images, momenta)


STEP = 4
RING = 8


def sweep_kernel(codes, scales, out, first, second, first_x, second_x, link, cross):
    step = pl.program_id(0)
    last = pl.num_programs(0) - 1
    zone = lax.axis_index("gz")
    zones = lax.axis_size("gz")
    finest = out.shape[1]
    half = finest // 2
    rest = finest - LANES
    wide_at = MARGIN
    tail_at = finest + 3 * MARGIN
    base = STEP * lax.rem(step, 2)
    piece = half // 3
    edge = iota((MARGIN, LANES), 1)
    low_first = (step == 0) & (zone == 0)
    high_last = (step == last) & (zone == zones - 1)

    def slot(o):
        return lax.rem(base + o + RING, RING)

    @pl.when(step == 0)
    def _():
        def wipe(at, _):
            first[at] = jnp.zeros(first.shape[1:], F32)
            second[at] = jnp.zeros(second.shape[1:], F32)
            first_x[at] = jnp.zeros(first_x.shape[1:], F32)
            second_x[at] = jnp.zeros(second_x.shape[1:], F32)
            return 0

        lax.fori_loop(0, RING, wipe, 0)
        row, column = iota(link.shape, 0), iota(link.shape, 1)
        low, high = jnp.minimum(row, column), jnp.maximum(row, column)
        split_at = LANES + rest
        near = (high == low + 1) & (high != split_at)
        link[...] = jnp.where(near, 1.0, 0.0).astype(BF16)
        meets = (low == LANES - 1) & (high == split_at)
        inner = (high == low + 1) & (high < LANES)
        cross[...] = jnp.where(meets | inner, 1.0, 0.0).astype(BF16)

    def put(ref, at, r, parts):
        top, bottom, tail = parts
        ref[at, pl.ds(wide_at + r, piece), :] = top
        ref[at, pl.ds(wide_at + half + r, piece), :] = bottom
        ref[at, pl.ds(tail_at + r, piece), :] = tail
        if r + piece == half:
            above = pltpu.roll(tail[piece - MARGIN :], LANES - rest, 1)
            ref[at, pl.ds(tail_at - MARGIN, MARGIN), :] = jnp.where(edge >= rest, above, 0.0)
        if r == 0:
            below = pltpu.roll(tail[:MARGIN], LANES - rest, 1)
            ref[at, pl.ds(tail_at + half, MARGIN), :] = jnp.where(edge < rest, below, 0.0)

    def lateral(ref, sums, at):
        top = ref[at, pl.ds(wide_at, half), :]
        bottom = ref[at, pl.ds(wide_at + half, half), :]
        tail = ref[at, pl.ds(tail_at, half), :]
        upper = dot(split(jnp.concatenate([top, tail], axis=1)), link[...])
        joint = dot(split(jnp.concatenate([bottom, tail], axis=1)), cross[...])
        upper = upper[:half] + upper[half:]
        joint = joint[:half] + joint[half:]
        sums[at, pl.ds(0, half), :] = upper[:, :LANES]
        sums[at, pl.ds(half, half), :] = joint[:, :LANES]
        sums[at, pl.ds(finest, half), :] = upper[:, LANES:] + joint[:, LANES:]

    def relax(ref, sums, o, r):
        here, before, after = slot(o), slot(o - 1), slot(o + 1)
        parts = []
        for at, side in (
            (wide_at + r, r), (wide_at + half + r, half + r), (tail_at + r, finest + r)
        ):
            rows = pl.ds(at, piece)
            total = (
                (ref[before, rows, :] + ref[after, rows, :])
                + (ref[here, pl.ds(at - 1, piece), :] + ref[here, pl.ds(at + 1, piece), :])
                + sums[here, pl.ds(side, piece), :]
            )
            parts.append(0.1 * ref[here, rows, :] + 0.15 * total)
        return parts

    for o in range(STEP):
        drop = low_first if o < 2 else high_last
        scale = jnp.where(drop, 0.0, scales[o][:1])
        for r in range(0, half, piece):
            at = (r, half + r, finest + r)
            put(first, slot(o), r, [codes[o, pl.ds(a, piece), :].astype(F32) * scale for a in at])
        lateral(first, first_x, slot(o))

    for o in range(-1, STEP - 1):
        for r in range(0, half, piece):
            parts = relax(first, first_x, o, r)
            if o == 1:
                parts = [jnp.where(low_first, 0.0, p) for p in parts]
            if o == 2:
                parts = [jnp.where(high_last, 0.0, p) for p in parts]
            put(second, slot(o), r, parts)
        lateral(second, second_x, slot(o))

    @pl.when(step >= 1)
    def _():
        for o in range(-2, STEP - 2):
            for r in range(0, half, piece):
                top, bottom, tail = relax(second, second_x, o, r)
                upper, lower = pl.ds(r, piece), pl.ds(half + r, piece)
                out[o + 2, upper, 0:LANES] = top
                out[o + 2, lower, 0:LANES] = bottom
                out[o + 2, upper, LANES:finest] = tail[:, :rest]
                out[o + 2, lower, LANES:finest] = pltpu.roll(tail, rest, 1)[:, :rest]


def sweeps(codes, scales, finest):
    planes, tall = codes.shape[0] - 4, codes.shape[1]
    ring = pltpu.VMEM((RING, tall + 4 * MARGIN, LANES), F32)
    return pl.pallas_call(
        sweep_kernel,
        grid=(planes // STEP + 1,),
        in_specs=[
            pl.BlockSpec((STEP, tall, LANES), lambda j: (j, 0, 0)),
            pl.BlockSpec((STEP, 8, LANES), lambda j: (j, 0, 0)),
        ],
        out_specs=pl.BlockSpec(
            (STEP, finest, finest), lambda j: (jnp.maximum(j - 1, 0), 0, 0)
        ),
        out_shape=jax.ShapeDtypeStruct((planes, finest, finest), F32),
        scratch_shapes=[
            ring,
            ring,
            pltpu.VMEM((RING, tall, LANES), F32),
            pltpu.VMEM((RING, tall, LANES), F32),
            pltpu.VMEM((2 * LANES, 2 * LANES), BF16),
            pltpu.VMEM((2 * LANES, 2 * LANES), BF16),
        ],
        compiler_params=pltpu.CompilerParams(dimension_semantics=("arbitrary",)),
    )(codes, scales)


def shards(images, momenta, assign):
    chips = lax.axis_size("subj") // 2
    if chips == 2:
        count = momenta.shape[0]
        home = jnp.arange(assign.shape[0], dtype=jnp.int32) // (2 * count)
        crossing = jnp.sum(((home == 0) & (assign // (2 * count) == 1)).astype(jnp.int32))
        codes, scales = lax.cond(
            crossing <= 2, functools.partial(fused, 1), functools.partial(fused, 2),
            assign, images, momenta,
        )
    else:
        codes, scales = fused(2, assign, images, momenta)
    return sweeps(codes, scales, images.shape[2])


def solution(mesh):
    return jax.shard_map(
        shards,
        mesh=mesh,
        in_specs=(P("subj", "gz", None, None), P("subj", "gz", None, None, None), P()),
        out_specs=P("gz", None, None),
        check_vma=False,
    )
```

```python
import functools

import jax
import jax.numpy as jnp
from jax import lax
from jax.experimental import pallas as pl
from jax.experimental.pallas import tpu as pltpu
from jax.sharding import PartitionSpec as P

LANES = 128
MARGIN = 8
TOP = 32767.0
LIMIT = 18.0
F32 = jnp.float32
BF16 = jnp.bfloat16


def split(value):
    high = value.astype(BF16)
    low = (value - high.astype(F32)).astype(BF16)
    return jnp.concatenate([high, low], axis=0)


def dot(a, b):
    return jnp.dot(a, b, preferred_element_type=F32)


def encode(packed):
    peak = jnp.max(jnp.abs(packed), axis=0, keepdims=True)
    peak = jnp.maximum(peak, 1e-30)
    code = jnp.floor(packed * (TOP / peak) + 0.5).astype(jnp.int16)
    return code, jnp.broadcast_to(peak * (1.0 / TOP), (8, LANES))


def iota(shape, axis):
    return lax.broadcasted_iota(jnp.int32, shape, axis)


def weight(fine_index, coarse_index, coarse):
    nearest = jnp.right_shift(fine_index, 1)
    farther = nearest + 2 * jnp.bitwise_and(fine_index, 1) - 1
    value = jnp.where(coarse_index == nearest, 0.75, jnp.where(coarse_index == farther, 0.25, 0.0))
    return jnp.where((coarse_index >= 0) & (coarse_index < coarse), value, 0.0).astype(BF16)


def slope(ahead, behind):
    return jnp.where(ahead, 0.5, jnp.where(behind, -0.5, 0.0)).astype(BF16)


def blur(gap):
    value = jnp.where(gap == 1, 0.25, jnp.where(gap == 2, 0.0625, 0.0))
    return jnp.where(gap == 0, 0.375, value).astype(BF16)


def make_tables(up_x, up_y, slope_x, slope_y, blur_x, blur_y):
    finest = up_y.shape[0]
    coarse = blur_x.shape[0]
    piece = LANES - coarse
    shape = (LANES, finest)
    lane, column = iota(shape, 0), iota(shape, 1)
    up_x[0] = weight(column, lane, coarse)
    for j in range(up_x.shape[0] - 1):
        index = jnp.where(lane >= coarse, lane - coarse + piece * j, -1)
        up_x[1 + j] = weight(column, index, coarse)
    shape = up_y.shape
    row, column = iota(shape, 0), iota(shape, 1)
    up_y[...] = weight(row, jnp.where(column >= coarse, column - coarse, column), coarse)
    slope_y[...] = slope(column == row + 1, column == row - 1)
    slope_x[...] = slope(row == column + 1, row == column - 1)
    shape = blur_x.shape
    blur_x[...] = jnp.where(
        iota(shape, 1) < coarse, blur(jnp.abs(iota(shape, 0) - iota(shape, 1))), 0.0
    ).astype(BF16)
    shape = blur_y.shape
    column = iota(shape, 1)
    column = jnp.where(column >= coarse, column - coarse, column)
    blur_y[...] = blur(jnp.abs(iota(shape, 0) - column))


def fused_kernel(
    messages, assign, images, momenta,
    codes, scales,
    up_x, up_y, slope_x, slope_y, blur_x, blur_y,
    ext, edges, hout, hin, img, vel, ymsg, fine, part, peer, ycode, yscale, mcode, mscale, xcode, xscale, zcode, zscale,
    lsem, hsend, hrecv, vsend, vrecv, qsend, qrecv, psend, precv, ysend, yrecv,
    gsend, grecv, xsend, xrecv, osem, zsend, zrecv,
):
    level = lax.axis_index("level")
    group = lax.axis_index("subj")
    zone = lax.axis_index("gz")
    groups = lax.axis_size("subj")
    zones = lax.axis_size("gz")
    chips = groups // 2
    chip = group // 2
    core = group % 2
    partner = 2 * chip + 1 - core
    up = level
    fine_slab, finest = images.shape[1], images.shape[2]
    slab, coarse = momenta.shape[1], momenta.shape[3]
    rows_half, planes_half = slab // 2, fine_slab // 2
    pairs = (rows_half + 2) // 2
    rows_block, planes_block = rows_half // 2, planes_half // 2
    half = finest // 2
    rest = finest - LANES
    piece = LANES - coarse

    to_zone = zone + 1 - 2 * level
    has_to = (to_zone >= 0) & (to_zone < zones)
    from_zone = zone - 1 + 2 * level
    has_from = (from_zone >= 0) & (from_zone < zones)
    me = (level, group, zone)
    mate = (level, partner, zone)
    across = (1 - level, group, zone)
    upper = (level, group, to_zone)
    peers = [(chip + d) % chips for d in range(1, chips)]

    def remote(src, dst, send, recv, device):
        return pltpu.make_async_remote_copy(
            src_ref=src, dst_ref=dst, send_sem=send, recv_sem=recv,
            device_id=device, device_id_type=pl.DeviceIdType.MESH,
        )

    load_mom = pltpu.make_async_copy(
        momenta.at[:, pl.ds(level * (rows_half - 3), rows_half + 3)],
        ext.at[:, pl.ds(3 - 3 * level, rows_half + 3)],
        lsem.at[0],
    )
    load_img = pltpu.make_async_copy(
        images.at[:, pl.ds(level * (planes_half - 1), planes_half + 1)],
        img.at[:, pl.ds(1 - level, planes_half + 1)],
        lsem.at[1],
    )
    load_edges = pltpu.make_async_copy(
        momenta.at[:, pl.ds((1 - level) * (slab - 3), 3)], edges, lsem.at[2]
    )
    load_edges.start()
    load_mom.start()
    barrier = pltpu.get_barrier_semaphore()

    def greet(device):
        pl.semaphore_signal(
            barrier, inc=1, device_id=device, device_id_type=pl.DeviceIdType.MESH
        )

    block = [(a, 2 * chip + b) for a in range(2) for b in range(2)]
    for a, b in block:
        @pl.when((a != level) | (b != group))
        def _(a=a, b=b):
            greet((a, b, zone))

    for other in peers:
        greet((level, 2 * other + core, zone))
    has_before = zone > 0
    has_after = zone < zones - 1

    @pl.when(has_before)
    def _():
        for a, b in block:
            greet((a, b, zone - 1))

    @pl.when(has_after)
    def _():
        for a, b in block:
            greet((a, b, zone + 1))

    make_tables(up_x, up_y, slope_x, slope_y, blur_x, blur_y)
    load_edges.wait()
    for s in range(2):
        for e in range(3):
            for k in range(3):
                code = jnp.floor(edges[s, e, k] * (TOP / LIMIT) + 0.5)
                hout[s, e, k] = jnp.clip(code, -TOP, TOP).astype(jnp.int16)
    pl.semaphore_wait(
        barrier,
        3 + len(peers)
        + 4 * has_before.astype(jnp.int32) + 4 * has_after.astype(jnp.int32),
    )

    halo_mom = remote(hout, hin, hsend.at[0], hrecv.at[0], upper)
    halo_img = remote(
        images.at[:, pl.ds((1 - level) * (fine_slab - 1), 1)],
        img.at[:, pl.ds(level * (planes_half + 1), 1)],
        hsend.at[1], hrecv.at[1], upper,
    )

    @pl.when(has_to)
    def _():
        halo_mom.start()
        halo_img.start()

    @pl.when(jnp.logical_not(has_from))
    def _():
        for s in range(2):
            for e in range(3):
                for k in range(3):
                    ext[s, level * (rows_half + 3) + e, k] = jnp.zeros((coarse, coarse), F32)
            img[s, level * (planes_half + 1)] = jnp.zeros((finest, finest), BF16)

    load_mom.wait()
    load_img.start()

    def pair_of(i):
        return i + (1 - up) * (pairs - 1 - 2 * i)

    strip = coarse // 2
    lane = iota((strip, LANES), 1)

    sources = [assign[2 * group + s] for s in range(2)]
    pieces = [(s, c) for s in range(2) for c in range(2)]

    def ranks(home):
        count = jnp.int32(0)
        places = {}
        for s, c in pieces:
            needed = jnp.bool_(False)
            for d in range(1, chips):
                there = (home + d) % chips
                for b in range(2):
                    row = assign[2 * (2 * there + b) + s]
                    needed = needed | (row == 2 * (2 * home + c) + s)
            places[s, c] = (needed, count)
            count = count + needed.astype(jnp.int32)
        return places

    def near_flag(s, c):
        return sources[s] == 2 * (2 * chip + c) + s

    if messages == 1:
        mine = ranks(chip)
        theirs_of = {other: ranks(peer_chip) for other, peer_chip in enumerate(peers)}

    def item_flag(s, other, n):
        if messages == 2:
            if n // 2 != s:
                return None
            return sources[s] == 2 * (2 * peers[other] + n % 2) + s
        flag = jnp.bool_(False)
        for c in range(2):
            needed, place = theirs_of[other][s, c]
            here = sources[s] == 2 * (2 * peers[other] + c) + s
            flag = flag | (here & needed & (place == n))
        return flag

    def near_send(t):
        return remote(vel.at[t, core], vel.at[t, core], vsend.at[t], vrecv.at[t], mate)

    def message_sends(t):
        part_of = ymsg.at[t, chip, :, pl.ds(strip * core, strip)]
        return [
            remote(
                part_of, part_of, qsend.at[t, n], qrecv.at[t, chip, core],
                (level, 2 * other + core, zone),
            )
            for n, other in enumerate(peers)
        ]

    def relay_sends(t):
        sends = []
        for n, other in enumerate(peers):
            part_of = ymsg.at[t, other, :, pl.ds(strip * core, strip)]
            sends.append(
                remote(
                    part_of, part_of, qsend.at[t, chips - 1 + n], qrecv.at[t, other, core], mate
                )
            )
        return sends

    def await_relayed(t):
        for other in peers:
            part_of = ymsg.at[t, other, :, pl.ds(strip * (1 - core), strip)]
            remote(
                part_of, part_of, qsend.at[t, 0], qrecv.at[t, other, 1 - core], mate
            ).wait_recv()

    def smooth(i):
        t = pair_of(i)
        planes = {}
        for r in range(2):
            row = zone * slab + level * rows_half - 1 + 2 * t + r
            keep = ((row >= 0) & (row < slab * zones)).astype(F32)
            for s in range(2):
                for k in range(3):
                    f = [ext[s, 2 * t + r + o, k] for o in range(5)]
                    value = (f[0] + f[4]) * 0.0625 + (f[1] + f[3]) * 0.25 + f[2] * 0.375
                    wide = dot(split(value), blur_x[...])
                    wide = (wide[:coarse] + wide[coarse:]) * keep
                    planes[6 * r + 3 * s + k] = dot(blur_y[...], split(wide))
        for p in range(12):
            vel[t, core, p] = planes[p].astype(BF16)

    def compose(t):
        rows = pl.ds(strip * core, strip)
        for m in range(messages):
            planes = []
            for r in range(2):
                for n in (2 * m, 2 * m + 1):
                    for k in range(3):
                        if messages == 2:
                            value = vel[t, n % 2, 6 * r + 3 * (n // 2) + k, rows]
                        else:
                            value = vel[t, 0, 6 * r + k, rows]
                            for s, c in pieces[1:]:
                                needed, place = mine[s, c]
                                value = jnp.where(
                                    needed & (place == n),
                                    vel[t, c, 6 * r + 3 * s + k, rows],
                                    value,
                                )
                        planes.append(value)
            for a in range(3):
                extra = planes[9 + a].astype(F32)
                for j in range(3):
                    turned = pltpu.roll(extra, coarse - piece * j, 1)
                    joined = jnp.where(lane < coarse, planes[3 * a + j].astype(F32), turned)
                    ymsg[t, chip, 9 * m + 3 * a + j, rows] = joined.astype(BF16)

    def share(i):
        t = pair_of(i)
        near_send(t).wait_recv()
        compose(t)
        for send in message_sends(t):
            send.start()

    def begin(i, _):
        smooth(i)
        near_send(pair_of(i)).start()

        @pl.when(i > 0)
        def _():
            share(i - 1)

        return 0

    lax.fori_loop(0, pairs - 2, begin, 0)
    share(pairs - 3)

    load_img.wait()

    def relay(t):
        for send in relay_sends(t):
            send.wait_recv()
            send.start()

    def raise_row(t, r, s):
        slot = lax.rem(2 * t + r, 4)
        p = 6 * r + 3 * s
        value = jnp.where(near_flag(s, 1), vel[t, 1, p : p + 3], vel[t, 0, p : p + 3])
        spread_out, spread_flag = None, jnp.bool_(False)
        for other in range(len(peers)):
            for n in range(2 * messages):
                flag = item_flag(s, other, n)
                if flag is None:
                    continue
                first = 9 * (n // 2)
                if r == 0 or n % 2 == 0:
                    at = first + 6 * r + 3 * (n % 2)
                    value = jnp.where(flag, ymsg[t, peers[other], at : at + 3], value)
                else:
                    group_of = ymsg[t, peers[other], first : first + 9]
                    if spread_out is None:
                        spread_out = group_of
                    else:
                        spread_out = jnp.where(flag, group_of, spread_out)
                    spread_flag = spread_flag | flag
        wide = dot(value.reshape(3 * coarse, LANES), up_x[0])
        for k in range(3):
            part_of = wide[coarse * k : coarse * (k + 1)]
            if spread_out is not None:
                total = dot(spread_out[3 * k], up_x[1])
                for j in range(1, 3):
                    total = total + dot(spread_out[3 * k + j], up_x[1 + j])
                part_of = jnp.where(spread_flag, total, part_of)
            fine[s, slot, k] = dot(up_y[...], split(part_of))

    chunk = finest // 4

    def warp_plane(row, z):
        middle = lax.rem(row, 4)
        outer = lax.rem(row + 3 + 2 * z, 4)
        plane = 2 * (row - 1) + z
        for r in range(0, finest, chunk):
            rows = pl.ds(r, chunk)
            total = None
            for s in range(2):
                image = img[s, plane + 1, rows, :]
                dx = dot(image, slope_x[...])
                dy = dot(slope_y[rows, :], img[s, plane + 1])
                back = img[s, plane, rows, :].astype(F32)
                ahead = img[s, plane + 2, rows, :].astype(F32)
                dz = (ahead - back) * 0.5
                near = (
                    fine[s, middle, 0, rows, :] * dx
                    + fine[s, middle, 1, rows, :] * dy
                    + fine[s, middle, 2, rows, :] * dz
                )
                side = (
                    fine[s, outer, 0, rows, :] * dx
                    + fine[s, outer, 1, rows, :] * dy
                    + fine[s, outer, 2, rows, :] * dz
                )
                value = image.astype(F32) - (0.75 * near + 0.25 * side)
                total = value if total is None else total + value
            part[plane, rows, :] = total[:, :LANES]
            place = rest * (r // half)
            part[plane, pl.ds(finest + r % half, chunk), place : place + rest] = total[:, LANES:]

    def chip_send(row):
        here = lax.rem(row, rows_block)
        return remote(
            part.at[pl.ds(2 * row, 2)], peer.at[pl.ds(2 * here, 2)],
            psend.at[here], precv.at[here], mate,
        )

    def sum_sends(here):
        sends = []
        for n, other in enumerate(peers):
            there = (level, 2 * other + core, zone)
            at = pl.ds(2 * here, 2)
            sends.append(
                remote(
                    ycode.at[chip, at], ycode.at[chip, at], ysend.at[0, here, n],
                    yrecv.at[0, here, chip], there,
                )
            )
            sends.append(
                remote(
                    yscale.at[chip, at], yscale.at[chip, at], ysend.at[1, here, n],
                    yrecv.at[1, here, chip], there,
                )
            )
        return sends

    def settle(row):
        here = lax.rem(row, rows_block)
        chip_send(row).wait_recv()
        for z in range(2):
            code, scale = encode(part[2 * row + z] + peer[2 * here + z])
            ycode[chip, 2 * here + z] = code
            yscale[chip, 2 * here + z] = scale
        for send in sum_sends(here):
            send.start()

    def row_at(n):
        n = jnp.where(n >= rows_half - 2, 2 * rows_half - 3 - n, n)
        return n + (1 - up) * (rows_half - 1 - 2 * n)

    def owned(row):
        return (row // rows_block) == core

    subjects = 2 * groups
    base = 2 + (2 * level + core) * planes_block
    away = 2 + (2 * (1 - level) + core) * planes_block

    def block_row(n):
        n = jnp.where(n >= rows_block - 2, 2 * rows_block - 3 - n, n)
        return n + (1 - up) * (rows_block - 1 - 2 * n)

    def spread(here):
        at = pl.ds(2 * here, 2)
        out = pl.ds(base + 2 * here, 2)
        sends = []
        for n, (src, cross, dst) in enumerate(((mcode, xcode, codes), (mscale, xscale, scales))):
            sends += [
                remote(src.at[at], cross.at[at], xsend.at[n, here], xrecv.at[n, here], across),
                remote(src.at[at], dst.at[out], gsend.at[n, 0, here], grecv.at[n, 0, here], mate),
                pltpu.make_async_copy(src.at[at], dst.at[out], osem.at[n, 0, here]),
            ]
        return sends

    def hand_on(here):
        at = pl.ds(2 * here, 2)
        out = pl.ds(away + 2 * here, 2)
        sends = []
        for n, (src, dst) in enumerate(((xcode, codes), (xscale, scales))):
            sends += [
                remote(src.at[at], dst.at[out], gsend.at[n, 1, here], grecv.at[n, 1, here], mate),
                pltpu.make_async_copy(src.at[at], dst.at[out], osem.at[n, 1, here]),
            ]
        return sends

    outermost = (level == core) & has_from
    edge_at = pl.ds(level * 2 * (rows_block - 1), 2)

    def edge_sends():
        sends = []
        for m, a in enumerate((1 - level, level)):
            for n, (src, dst) in enumerate(((mcode, zcode), (mscale, zscale))):
                sends.append(
                    remote(
                        src.at[edge_at], dst, zsend.at[n, m], zrecv.at[n, 0],
                        (a, group, from_zone),
                    )
                )
        return sends

    has_direct = jnp.where(core == 1, zone, zones - 1 - zone) > 0
    has_relayed = jnp.where(core == 1, zones - 1 - zone, zone) > 0
    direct_out = pl.ds((1 - core) * (fine_slab + 2), 2)
    relayed_out = pl.ds(core * (fine_slab + 2), 2)

    def edge_hands():
        sends = []
        for n, (src, dst) in enumerate(((zcode, codes), (zscale, scales))):
            out = dst.at[direct_out]
            sends += [
                remote(src, out, zsend.at[n, 2], zrecv.at[n, 1], mate),
                pltpu.make_async_copy(src, out, osem.at[n, 2, 0]),
            ]
        return sends

    def publish(here):
        at = pl.ds(2 * here, 2)
        for other in peers:
            for n, buffer in enumerate((ycode, yscale)):
                remote(
                    buffer.at[other, at], buffer.at[other, at], ysend.at[n, here, 0],
                    yrecv.at[n, here, other], me,
                ).wait_recv()
        for z in range(2):
            plane = 2 * here + z
            value = ycode[0, plane].astype(F32) * yscale[0, plane][:1]
            for other in range(1, chips):
                value = value + ycode[other, plane].astype(F32) * yscale[other, plane][:1]
            code, scale = encode(value * (1.0 / subjects))
            mcode[plane] = code
            mscale[plane] = scale
        for send in spread(here):
            send.start()

    is_first = core == 1 - up
    early = min(4, rows_block)
    halo_at = (pairs - 3) // 2
    relay(pair_of(0))

    def main(i, _):
        t = pair_of(i)

        @pl.when((i == halo_at) & has_from)
        def _():
            halo_mom.wait_recv()
            for s in range(2):
                for e in range(3):
                    for k in range(3):
                        value = hin[s, e, k].astype(F32) * (LIMIT / TOP)
                        ext[s, level * (rows_half + 3) + e, k] = value

        late = (i == halo_at) | (i == halo_at + 1)
        late_pair = pairs - 2 + i - halo_at

        @pl.when(late)
        def _():
            smooth(late_pair)
            near_send(pair_of(late_pair)).start()

        @pl.when(i < pairs - 1)
        def _():
            relay(pair_of(i + 1))

        await_relayed(t)
        for r in range(2):
            for s in range(2):
                raise_row(t, r, s)

        @pl.when(late)
        def _():
            share(late_pair)

        @pl.when((i == pairs - 1) & has_from)
        def _():
            halo_img.wait_recv()

        @pl.when(i >= 1)
        def _():
            def step(w, _):
                n = 2 * (i - 1) + w // 2
                row = row_at(n)
                warp_plane(row + 1, lax.rem(w, 2))

                @pl.when(lax.rem(w, 2) == 1)
                def _():
                    @pl.when(jnp.logical_not(owned(row)))
                    def _():
                        chip_send(row).start()

                    prior = row_at(jnp.maximum(n - 1, 0))

                    @pl.when((n > 0) & owned(prior))
                    def _():
                        settle(prior)

                @pl.when((i == pairs - 1) & is_first & (w < early))
                def _():
                    publish(block_row(w))

                return 0

            lax.fori_loop(0, 4, step, 0)

        return 0

    lax.fori_loop(0, pairs, main, 0)

    @pl.when(jnp.logical_not(is_first))
    def _():
        settle(row_at(rows_half - 1))

    def finish(n, _):
        @pl.when(jnp.logical_not(is_first) | (n >= early))
        def _():
            publish(block_row(n))

        @pl.when(outermost & (n == rows_block - 2))
        def _():
            for send in edge_sends():
                send.start()

        return 0

    lax.fori_loop(0, rows_block, finish, 0)

    def hand(n, _):
        here = rows_block - 1 - block_row(n)
        first, second = spread(here)[0], spread(here)[3]
        first.wait_recv()
        second.wait_recv()
        for send in hand_on(here):
            send.start()
        return 0

    lax.fori_loop(0, rows_block - 2, hand, 0)

    @pl.when(has_direct)
    def _():
        for n, src in enumerate((zcode, zscale)):
            remote(src, src, zsend.at[n, 0], zrecv.at[n, 0], me).wait_recv()
        for send in edge_hands():
            send.start()

    lax.fori_loop(rows_block - 2, rows_block, hand, 0)

    @pl.when(has_to)
    def _():
        halo_mom.wait_send()
        halo_img.wait_send()

    def drain_velocity(t, _):
        near_send(t).wait_send()
        for send in message_sends(t) + relay_sends(t):
            send.wait_send()
        return 0

    lax.fori_loop(0, pairs, drain_velocity, 0)

    def drain_rows(here, _):
        chip_send((1 - core) * rows_block + here).wait_send()
        for send in sum_sends(here):
            send.wait_send()
        for n, send in enumerate(spread(here)):
            if n % 3 == 0:
                send.wait_send()
            else:
                send.wait()
        for send in hand_on(here):
            send.wait()
        return 0

    lax.fori_loop(0, rows_block, drain_rows, 0)

    @pl.when(outermost)
    def _():
        for send in edge_sends():
            send.wait_send()

    @pl.when(has_direct)
    def _():
        for n, send in enumerate(edge_hands()):
            if n % 2 == 0:
                send.wait_send()
            else:
                send.wait()

    @pl.when(has_relayed)
    def _():
        for n, dst in enumerate((codes, scales)):
            out = dst.at[relayed_out]
            remote(out, out, zsend.at[n, 0], zrecv.at[n, 1], me).wait_recv()


def fused(messages, assign, images, momenta):
    groups = lax.axis_size("subj")
    chips = groups // 2
    fine_slab, finest = images.shape[1], images.shape[2]
    slab, coarse = momenta.shape[1], momenta.shape[3]
    rows_half, planes_half = slab // 2, fine_slab // 2
    pairs = (rows_half + 2) // 2
    rows_block, planes_block = rows_half // 2, planes_half // 2
    tall = finest + finest // 2
    tables = 1 + coarse // (LANES - coarse)
    dma = pltpu.SemaphoreType.DMA
    hbm = pl.BlockSpec(memory_space=pl.ANY)
    scratch = [
        pltpu.VMEM((tables, LANES, finest), BF16),
        pltpu.VMEM((finest, finest), BF16),
        pltpu.VMEM((finest, finest), BF16),
        pltpu.VMEM((finest, finest), BF16),
        pltpu.VMEM((coarse, LANES), BF16),
        pltpu.VMEM((coarse, 2 * coarse), BF16),
        pltpu.VMEM((2, rows_half + 6, 3, coarse, coarse), F32),
        pltpu.VMEM((2, 3, 3, coarse, coarse), F32),
        pltpu.VMEM((2, 3, 3, coarse, coarse), jnp.int16),
        pltpu.VMEM((2, 3, 3, coarse, coarse), jnp.int16),
        pltpu.VMEM((2, planes_half + 2, finest, finest), BF16),
        pltpu.VMEM((pairs, 2, 12, coarse, LANES), BF16),
        pltpu.VMEM((pairs, chips, 9 * messages, coarse, LANES), BF16),
        pltpu.VMEM((2, 4, 3, finest, finest), F32),
        pltpu.VMEM((planes_half, tall, LANES), F32),
        pltpu.VMEM((planes_block, tall, LANES), F32),
        pltpu.VMEM((chips, planes_block, tall, LANES), jnp.int16),
        pltpu.VMEM((chips, planes_block, 8, LANES), F32),
        pltpu.VMEM((planes_block, tall, LANES), jnp.int16),
        pltpu.VMEM((planes_block, 8, LANES), F32),
        pltpu.VMEM((planes_block, tall, LANES), jnp.int16),
        pltpu.VMEM((planes_block, 8, LANES), F32),
        pltpu.VMEM((2, tall, LANES), jnp.int16),
        pltpu.VMEM((2, 8, LANES), F32),
        dma((3,)),
        dma((2,)),
        dma((2,)),
        dma((pairs,)),
        dma((pairs,)),
        dma((pairs, 2 * (chips - 1))),
        dma((pairs, chips, 2)),
        dma((rows_block,)),
        dma((rows_block,)),
        dma((2, rows_block, max(chips - 1, 1))),
        dma((2, rows_block, chips)),
        dma((2, 2, rows_block)),
        dma((2, 2, rows_block)),
        dma((2, rows_block)),
        dma((2, rows_block)),
        dma((2, 3, rows_block)),
        dma((2, 3)),
        dma((2, 2)),
    ]
    return pl.pallas_call(
        functools.partial(fused_kernel, messages),
        out_shape=(
            jax.ShapeDtypeStruct((fine_slab + 4, tall, LANES), jnp.int16),
            jax.ShapeDtypeStruct((fine_slab + 4, 8, LANES), F32),
        ),
        in_specs=[pl.BlockSpec(memory_space=pltpu.SMEM), hbm, hbm],
        out_specs=(hbm, hbm),
        scratch_shapes=scratch,
        compiler_params=pltpu.CompilerParams(
            collective_id=messages, has_side_effects=True, vmem_limit_bytes=60 * 1024 * 1024
        ),
    )(assign, images, momenta)


STEP = 4
RING = 8


def sweep_kernel(codes, scales, out, first, second, first_x, second_x, link, cross):
    step = pl.program_id(0)
    last = pl.num_programs(0) - 1
    zone = lax.axis_index("gz")
    zones = lax.axis_size("gz")
    finest = out.shape[1]
    half = finest // 2
    rest = finest - LANES
    wide_at = MARGIN
    tail_at = finest + 3 * MARGIN
    base = STEP * lax.rem(step, 2)
    piece = half // 3
    edge = iota((MARGIN, LANES), 1)
    low_first = (step == 0) & (zone == 0)
    high_last = (step == last) & (zone == zones - 1)

    def slot(o):
        return lax.rem(base + o + RING, RING)

    @pl.when(step == 0)
    def _():
        def wipe(at, _):
            first[at] = jnp.zeros(first.shape[1:], F32)
            second[at] = jnp.zeros(second.shape[1:], F32)
            first_x[at] = jnp.zeros(first_x.shape[1:], F32)
            second_x[at] = jnp.zeros(second_x.shape[1:], F32)
            return 0

        lax.fori_loop(0, RING, wipe, 0)
        row, column = iota(link.shape, 0), iota(link.shape, 1)
        low, high = jnp.minimum(row, column), jnp.maximum(row, column)
        split_at = LANES + rest
        near = (high == low + 1) & (high != split_at)
        link[...] = jnp.where(near, 1.0, 0.0).astype(BF16)
        meets = (low == LANES - 1) & (high == split_at)
        inner = (high == low + 1) & (high < LANES)
        cross[...] = jnp.where(meets | inner, 1.0, 0.0).astype(BF16)

    def put(ref, at, r, parts):
        top, bottom, tail = parts
        ref[at, pl.ds(wide_at + r, piece), :] = top
        ref[at, pl.ds(wide_at + half + r, piece), :] = bottom
        ref[at, pl.ds(tail_at + r, piece), :] = tail
        if r + piece == half:
            above = pltpu.roll(tail[piece - MARGIN :], LANES - rest, 1)
            ref[at, pl.ds(tail_at - MARGIN, MARGIN), :] = jnp.where(edge >= rest, above, 0.0)
        if r == 0:
            below = pltpu.roll(tail[:MARGIN], LANES - rest, 1)
            ref[at, pl.ds(tail_at + half, MARGIN), :] = jnp.where(edge < rest, below, 0.0)

    def lateral(ref, sums, at):
        top = ref[at, pl.ds(wide_at, half), :]
        bottom = ref[at, pl.ds(wide_at + half, half), :]
        tail = ref[at, pl.ds(tail_at, half), :]
        upper = dot(split(jnp.concatenate([top, tail], axis=1)), link[...])
        joint = dot(split(jnp.concatenate([bottom, tail], axis=1)), cross[...])
        upper = upper[:half] + upper[half:]
        joint = joint[:half] + joint[half:]
        sums[at, pl.ds(0, half), :] = upper[:, :LANES]
        sums[at, pl.ds(half, half), :] = joint[:, :LANES]
        sums[at, pl.ds(finest, half), :] = upper[:, LANES:] + joint[:, LANES:]

    def relax(ref, sums, o, r):
        here, before, after = slot(o), slot(o - 1), slot(o + 1)
        parts = []
        for at, side in (
            (wide_at + r, r), (wide_at + half + r, half + r), (tail_at + r, finest + r)
        ):
            rows = pl.ds(at, piece)
            total = (
                (ref[before, rows, :] + ref[after, rows, :])
                + (ref[here, pl.ds(at - 1, piece), :] + ref[here, pl.ds(at + 1, piece), :])
                + sums[here, pl.ds(side, piece), :]
            )
            parts.append(0.1 * ref[here, rows, :] + 0.15 * total)
        return parts

    for o in range(STEP):
        drop = low_first if o < 2 else high_last
        scale = jnp.where(drop, 0.0, scales[o][:1])
        for r in range(0, half, piece):
            at = (r, half + r, finest + r)
            put(first, slot(o), r, [codes[o, pl.ds(a, piece), :].astype(F32) * scale for a in at])
        lateral(first, first_x, slot(o))

    for o in range(-1, STEP - 1):
        for r in range(0, half, piece):
            parts = relax(first, first_x, o, r)
            if o == 1:
                parts = [jnp.where(low_first, 0.0, p) for p in parts]
            if o == 2:
                parts = [jnp.where(high_last, 0.0, p) for p in parts]
            put(second, slot(o), r, parts)
        lateral(second, second_x, slot(o))

    @pl.when(step >= 1)
    def _():
        for o in range(-2, STEP - 2):
            for r in range(0, half, piece):
                top, bottom, tail = relax(second, second_x, o, r)
                upper, lower = pl.ds(r, piece), pl.ds(half + r, piece)
                out[o + 2, upper, 0:LANES] = top
                out[o + 2, lower, 0:LANES] = bottom
                out[o + 2, upper, LANES:finest] = tail[:, :rest]
                out[o + 2, lower, LANES:finest] = pltpu.roll(tail, rest, 1)[:, :rest]


def sweeps(codes, scales, finest):
    planes, tall = codes.shape[0] - 4, codes.shape[1]
    ring = pltpu.VMEM((RING, tall + 4 * MARGIN, LANES), F32)
    return pl.pallas_call(
        sweep_kernel,
        grid=(planes // STEP + 1,),
        in_specs=[
            pl.BlockSpec((STEP, tall, LANES), lambda j: (j, 0, 0)),
            pl.BlockSpec((STEP, 8, LANES), lambda j: (j, 0, 0)),
        ],
        out_specs=pl.BlockSpec(
            (STEP, finest, finest), lambda j: (jnp.maximum(j - 1, 0), 0, 0)
        ),
        out_shape=jax.ShapeDtypeStruct((planes, finest, finest), F32),
        scratch_shapes=[
            ring,
            ring,
            pltpu.VMEM((RING, tall, LANES), F32),
            pltpu.VMEM((RING, tall, LANES), F32),
            pltpu.VMEM((2 * LANES, 2 * LANES), BF16),
            pltpu.VMEM((2 * LANES, 2 * LANES), BF16),
        ],
        compiler_params=pltpu.CompilerParams(dimension_semantics=("arbitrary",)),
    )(codes, scales)


def shards(images, momenta, assign):
    chips = lax.axis_size("subj") // 2
    if chips == 2:
        count = momenta.shape[0]
        home = jnp.arange(assign.shape[0], dtype=jnp.int32) // (2 * count)
        crossing = jnp.sum(((home == 0) & (assign // (2 * count) == 1)).astype(jnp.int32))
        codes, scales = lax.cond(
            crossing <= 2, functools.partial(fused, 1), functools.partial(fused, 2),
            assign, images, momenta,
        )
    else:
        codes, scales = fused(2, assign, images, momenta)
    return sweeps(codes, scales, images.shape[2])


def solution(mesh):
    return jax.shard_map(
        shards,
        mesh=mesh,
        in_specs=(P("subj", "gz", None, None), P("subj", "gz", None, None, None), P()),
        out_specs=P("gz", None, None),
        check_vma=False,
    )
```
